32 devices in a mesh: group: 4 (over y, x), replica: 8 (over z, core).
Axes of the slice: x: 2, y: 2, z: 4, core: 2. Of those that a mesh axis runs over, the one named last changes fastest.
Arguments:
- tokens: bfloat16 [8, 1024, 2048], P('replica', 'group'), may hold values from -30 to 30
- segments: int32 [8, 1024], P('replica'), may hold values from 0 to 3, as said below
- positions: int32 [8, 1024], P('replica', 'group'), may hold values from 0 to 2047, as said below
- norm_in: bfloat16 [2048], P('group'), may hold values from 0.5 to 2
- w_qkv: bfloat16 [2048, 3072], P('group'), may hold values from -4 to 4
- w_out: bfloat16 [2048, 2048], P('group'), may hold values from -1 to 1
- norm_mid: bfloat16 [2048], P('group'), may hold values from 0.5 to 2
- w_in: bfloat16 [8192, 2, 2048], P('group'), may hold values from -0.125 to 0.125
- w_down: bfloat16 [8192, 2048], P('group'), may hold values from -0.0625 to 0.0625
- cotangent: bfloat16 [8, 1024, 2048], P('replica', 'group'), may hold values from -6 to 6
Outputs:
- output: bfloat16 [8, 1024, 2048], P('replica', 'group')
- grad_tokens: bfloat16 [8, 1024, 2048], P('replica', 'group')
- grad_norm_in: float32 [2048], P('group')
- grad_w_qkv: float32 [2048, 3072], P('group')
- grad_w_out: float32 [2048, 2048], P('group')
- grad_norm_mid: float32 [2048], P('group')
- grad_w_in: float32 [8192, 2, 2048], P('group')
- grad_w_down: float32 [8192, 2048], P('group')
The draws below stay inside these ranges and needn't reach their ends.
Inputs may be any that keep to these rules, and one draw needn't show every extreme that they name: `segments`: document numbers start at 0 on each sequence's first token, never fall along a sequence and end at 3; the first document of a sequence holds at least half of its tokens. Within a document the positions rise by one from token to token; the last document of each sequence starts at position 0.
All inputs are finite; a program needn't handle non-finite values.
Results may differ from the reference program's by a relative error of at most 0.019.
Values may be sent and summed in bfloat16 or wider, within the bound.
A program may use at most 384 MiB of HBM per device.

```python
import math
import jax
import jax.numpy as jnp
from jax import lax

D = 2048
HEADS = 32
KV_HEADS = 8
HEAD = 64
FF = 8192
CUTS = 3
SEQ = 1024
SEQS = 8
KVW = 512


def packing(key):

    def one_sequence(sub):
        first_key, rest_key, offset_key = jax.random.split(sub, 3)
        first_cut = jax.random.randint(first_key, (1,), SEQ // 2, 3 * SEQ // 4)
        rest_cuts = jax.random.randint(rest_key, (CUTS - 1,), first_cut[0], SEQ)
        cuts = jnp.concatenate([first_cut, rest_cuts]).astype(jnp.int32)
        index = jnp.arange(SEQ, dtype=jnp.int32)
        passed = cuts[None, :] <= index[:, None]
        seg_ids = jnp.sum(passed.astype(jnp.int32), axis=1)
        starts = jnp.max(jnp.where(passed, cuts[None, :], 0), axis=1)
        offsets = jax.random.randint(offset_key, (CUTS + 1,), 0, SEQ)
        labels = jnp.arange(CUTS + 1, dtype=jnp.int32)
        offsets = jnp.where(labels == CUTS, 0, offsets)
        offsets = jnp.where(labels == 0, 2 * SEQ - first_cut[0], offsets)
        picked = jnp.sum(jnp.where(seg_ids[:, None] == labels[None, :], offsets[None, :], 0), axis=1)
        return (seg_ids, (picked + index - starts).astype(jnp.int32))
    keys = jax.random.split(key, SEQS)
    return jax.vmap(one_sequence)(keys)


def draw_segments(key, part):
    return packing(jax.random.fold_in(key, 11))[0]


def draw_positions(key, part):
    return packing(jax.random.fold_in(key, 11))[1]


def draw_tokens(key, part):
    row_key, col_key, base_key = jax.random.split(jax.random.fold_in(key, 5), 3)
    row_scale = jnp.exp(jax.random.uniform(row_key, (SEQS, SEQ, 1), jnp.float32, math.log(0.3), math.log(3.0)))
    col_scale = jnp.exp(jax.random.uniform(col_key, (D,), jnp.float32, math.log(0.3), math.log(3.0)))
    base = jnp.clip(jax.random.normal(base_key, (SEQS, SEQ, D), jnp.float32), -4.0, 4.0)
    return jnp.clip(base * row_scale * col_scale, -30.0, 30.0).astype(jnp.bfloat16)


def draw_w_qkv(key, part):
    base_key = jax.random.fold_in(jax.random.fold_in(key, 3), 0)
    scale = D ** (-0.5)
    base = jnp.clip(jax.random.normal(base_key, (D, D + 2 * KV_HEADS * HEAD), jnp.float32), -4.0, 4.0) * scale
    return jnp.clip(base, -4.0, 4.0).astype(jnp.bfloat16)


def raised(values, own_key, source, target, parts, factor):
    def block_of(dim):
        return (jnp.arange(values.shape[dim]) // (values.shape[dim] // parts)).reshape((-1,) + (1,) * (values.ndim - 1 - dim))

    one_side = jax.random.permutation(own_key, parts)[block_of(target)]
    other_side = (block_of(target) + parts // 2) % parts
    return jnp.where((block_of(source) == one_side) | (block_of(source) == other_side), factor * values, values)


def level_of(stream_key, shape, cuts, smallest, largest):
    def one(dim, parts):
        steps = jax.random.uniform(jax.random.fold_in(jax.random.fold_in(stream_key, 6), dim), (parts,), jnp.float32, smallest / len(cuts), largest / len(cuts))
        return jnp.repeat(jnp.exp(steps), shape[dim] // parts).reshape((-1,) + (1,) * (len(shape) - dim - 1))

    factor_of = one(*cuts[0])
    for cut in cuts[1:]:
        factor_of = factor_of * one(*cut)
    return factor_of


def scatter_about(key, dims, spread, bound, pieces=(), kind=jnp.bfloat16):
    drawn = spread * jax.random.normal(key, dims, jnp.float32)
    if pieces:
        drawn = drawn * level_of(key, dims, pieces, -0.22, 0.18)
    return jnp.clip(drawn, -bound, bound).astype(kind)


def heavy_noise(own_key, shape, width, limit, shards, heavy, kind=jnp.bfloat16):
    values = width * jax.random.normal(own_key, shape, jnp.float32)
    if shards:
        values = values * level_of(own_key, shape, shards, -0.22, 0.18)
    return jnp.clip(raised(values, jax.random.fold_in(own_key, 3), *heavy), -limit, limit).astype(kind)


def setup_inputs(seed: int = 0) -> dict:
    seeds = jax.random.split(jax.random.key(seed), 11)
    tokens = draw_tokens(jax.random.fold_in(seeds[10], 71), 0)
    segments = draw_segments(jax.random.fold_in(seeds[10], 71), 0)
    positions = draw_positions(jax.random.fold_in(seeds[10], 71), 0)
    norm_in = jnp.clip(jnp.exp(math.log(2.0) - 1.3862944 * jax.random.uniform(seeds[3], (D,), jnp.float32) ** level_of(seeds[3], (D,), ((0, 4),), -0.2, 0.2)), 0.5, 2.0).astype(jnp.bfloat16)
    w_qkv = draw_w_qkv(jax.random.fold_in(seeds[10], 71), 0)
    w_out = scatter_about(seeds[5], (D, D), (D // 64) ** -0.5, 1.0, ((0, 4),))
    norm_mid = jnp.clip(jnp.exp(math.log(2.0) - 1.3862944 * jax.random.uniform(seeds[6], (D,), jnp.float32) ** level_of(seeds[6], (D,), ((0, 4),), -0.2, 0.2)), 0.5, 2.0).astype(jnp.bfloat16)
    w_in = scatter_about(seeds[7], (FF, 2, D), D ** -0.5, 0.125, ((0, 4),))
    w_down = scatter_about(seeds[8], (FF, D), FF ** -0.5, 0.0625, ((0, 4),))
    cotangent = heavy_noise(seeds[9], (SEQS, SEQ, D), 1.0, 6.0, ((0, 8), (1, 4)), (0, 2, 8, 2.0))
    return dict(tokens=tokens, segments=segments, positions=positions, norm_in=norm_in, w_qkv=w_qkv, w_out=w_out, norm_mid=norm_mid, w_in=w_in, w_down=w_down, cotangent=cotangent)


EPS = 1e-05
ROPE_BASE = 500000.0
ROPE_FACTOR = 32.0
LOW_FACTOR = 1.0
HIGH_FACTOR = 4.0
OLD_CONTEXT = 8192.0
HIGH = lax.Precision.HIGHEST

@jax.custom_vjp
def low(v):
    return lax.optimization_barrier(v.astype(jnp.bfloat16)).astype(jnp.float32)

@jax.custom_vjp
def low_back(v):
    return v

def low_keep(v):
    return (low(v), None)

def low_pass(kept, grad):
    return (grad,)

def back_keep(v):
    return (v, None)

def back_low(kept, grad):
    return (low(grad),)
low.defvjp(low_keep, low_pass)
low_back.defvjp(back_keep, back_low)

def rope_frequency(head_size):
    half = head_size // 2
    exponent = jnp.arange(half).astype(jnp.float32) * (2.0 / head_size)
    frequency = jnp.power(jnp.float32(ROPE_BASE), -exponent)
    wavelength = 2.0 * math.pi / frequency
    smooth = (OLD_CONTEXT / wavelength - LOW_FACTOR) / (HIGH_FACTOR - LOW_FACTOR)
    blended = (1.0 - smooth) * frequency / ROPE_FACTOR + smooth * frequency
    slow = jnp.where(wavelength > OLD_CONTEXT / LOW_FACTOR, frequency / ROPE_FACTOR, blended)
    return jnp.where(wavelength < OLD_CONTEXT / HIGH_FACTOR, frequency, slow)

def rope_tables(position, head_size):
    frequency = rope_frequency(head_size)
    angle = position.astype(jnp.float32)[:, None] * frequency[None, :]
    return (jnp.cos(angle), jnp.sin(angle))

def rotate(values, cosine, sine, sign):
    half = values.shape[-1] // 2
    first = values[..., :half]
    second = values[..., half:]
    cos_part = cosine[:, None, :]
    sin_part = sine[:, None, :] * sign
    return jnp.concatenate([first * cos_part - second * sin_part, second * cos_part + first * sin_part], axis=-1)

def layer(inputs, norm_in, w_qkv, w_out, norm_mid, w_in, w_down, seg_ids, position):
    length = inputs.shape[0]
    repeat = HEADS // KV_HEADS
    scale = 1.0 / math.sqrt(HEAD)
    scale_in = lax.rsqrt(lax.optimization_barrier(jnp.mean(inputs * inputs, axis=-1, keepdims=True)) + EPS)
    normed_in = low(inputs * scale_in * norm_in)
    projected = low_back(jnp.dot(normed_in, w_qkv, precision=HIGH))
    cosine, sine = rope_tables(position, HEAD)
    queries = low(rotate(projected[:, :D].reshape(length, HEADS, HEAD), cosine, sine, 1.0))
    keys = low(rotate(projected[:, D:D + KVW].reshape(length, KV_HEADS, HEAD), cosine, sine, 1.0))
    values = low(projected[:, D + KVW:].reshape(length, KV_HEADS, HEAD))
    index = jnp.arange(length, dtype=jnp.int32)
    mask = (index[None, :] <= index[:, None]) & (seg_ids[:, None] == seg_ids[None, :])
    grouped_q = jnp.moveaxis(queries.reshape(length, KV_HEADS, repeat, HEAD), 1, 0)
    grouped_k = jnp.moveaxis(keys, 1, 0)
    grouped_v = jnp.moveaxis(values, 1, 0)

    def one_head(items):
        query_head, key_head, value_head = items
        scores = low_back(jnp.einsum('trd,sd->rts', query_head, key_head, precision=HIGH) * scale)
        scores = jnp.where(mask[None], scores, -jnp.inf)
        row_max = lax.optimization_barrier(jnp.max(scores, axis=-1, keepdims=True))
        expo = jnp.exp(scores - row_max)
        probs = expo / lax.optimization_barrier(jnp.sum(expo, axis=-1, keepdims=True))
        return jnp.einsum('rts,sd->trd', low(probs), value_head, precision=HIGH)
    mixed = lax.map(jax.checkpoint(one_head), (grouped_q, grouped_k, grouped_v))
    attended = low(low_back(jnp.moveaxis(mixed, 0, 1).reshape(length, D)))
    branch = low_back(jnp.dot(attended, w_out, precision=HIGH))
    middle = inputs + branch
    scale_mid = lax.rsqrt(lax.optimization_barrier(jnp.mean(middle * middle, axis=-1, keepdims=True)) + EPS)
    normed = low(middle * scale_mid * norm_mid)
    gate = low_back(jnp.einsum('td,fd->tf', normed, w_in[:, 0, :], precision=HIGH))
    up_part = low_back(jnp.einsum('td,fd->tf', normed, w_in[:, 1, :], precision=HIGH))
    hidden = low(gate * jax.nn.sigmoid(gate) * up_part)
    feed = low_back(jnp.dot(hidden, w_down, precision=HIGH))
    return middle + feed

def reference(tokens, segments, positions, norm_in, w_qkv, w_out, norm_mid, w_in, w_down, cotangent):
    weights = tuple((w.astype(jnp.float32) for w in (norm_in, w_qkv, w_out, norm_mid, w_in, w_down)))
    zeros = tuple((jnp.zeros_like(w) for w in weights))

    def per_sequence(totals, items):
        inputs, seg_ids, position, grad_out = items

        def apply(input_float, *params):
            return layer(input_float, *params, seg_ids, position)
        result, pullback = jax.vjp(apply, inputs.astype(jnp.float32), *weights)
        grads = pullback(grad_out.astype(jnp.float32))
        updated = tuple((a + b for a, b in zip(totals, grads[1:])))
        return (updated, (result.astype(jnp.bfloat16), grads[0].astype(jnp.bfloat16)))
    totals, (outputs, grad_tokens) = lax.scan(per_sequence, zeros, (tokens, segments, positions, cotangent))
    return (outputs, grad_tokens, totals[0], totals[1], totals[2], totals[3], totals[4], totals[5])
```

```python
import functools
import math

import jax
import jax.numpy as jnp
from jax import lax
from jax.experimental import pallas as pl
from jax.experimental.pallas import tpu as pltpu
from jax.sharding import PartitionSpec as P

HEAD = 64
EPS = 1e-05
ROPE_BASE = 500000.0
ROPE_FACTOR = 32.0
LOW_FACTOR = 1.0
HIGH_FACTOR = 4.0
OLD_CONTEXT = 8192.0
BF = jnp.bfloat16
F32 = jnp.float32
NEG = -1e30

CHUNK = 256


def rope_frequency(head_size):
    half = head_size // 2
    exponent = jnp.arange(half).astype(jnp.float32) * (2.0 / head_size)
    frequency = jnp.power(jnp.float32(ROPE_BASE), -exponent)
    wavelength = 2.0 * math.pi / frequency
    smooth = (OLD_CONTEXT / wavelength - LOW_FACTOR) / (HIGH_FACTOR - LOW_FACTOR)
    blended = (1.0 - smooth) * frequency / ROPE_FACTOR + smooth * frequency
    slow = jnp.where(wavelength > OLD_CONTEXT / LOW_FACTOR, frequency / ROPE_FACTOR, blended)
    return jnp.where(wavelength < OLD_CONTEXT / HIGH_FACTOR, frequency, slow)


def rope_tables(position, head_size):
    frequency = rope_frequency(head_size)
    angle = position.astype(jnp.float32)[:, None] * frequency[None, :]
    return (jnp.cos(angle), jnp.sin(angle))


def rms_scale(values):
    return lax.rsqrt(jnp.mean(values * values, axis=-1, keepdims=True) + EPS)


def norm_backward(grad_normed, unit, scale, gain):
    grad_unit = grad_normed * gain
    grad_input = scale * (grad_unit - unit * jnp.mean(grad_unit * unit, axis=-1, keepdims=True))
    return (grad_input, jnp.sum(grad_normed * unit, axis=0))


def mm(a, b, ca, cb):
    return lax.dot_general(a, b, (((ca,), (cb,)), ((), ())), preferred_element_type=F32)


def swap(value, axis, mask):
    return lax.ppermute(value, axis, [(i, i ^ mask) for i in range(lax.axis_size(axis))])


def bit_list(number):
    return [1 << b for b in range(number.bit_length()) if number >> b & 1]


def pieces_of(rows, number):
    bits = bit_list(number)
    while rows % (16 * len(bits)):
        bits = bits[:-1]
    step = rows // len(bits)
    return [(bit, i * step, step) for i, bit in enumerate(bits)]


def gather_blocks(own, axis):
    blocks = [own]
    for s in range(1, lax.axis_size(axis)):
        parts = [
            swap(blocks[s ^ bit][start : start + size], axis, bit)
            for bit, start, size in pieces_of(own.shape[0], s)
        ]
        blocks.append(parts[0] if len(parts) == 1 else jnp.concatenate(parts, axis=0))
    return blocks


def scatter_sum(terms, axis):
    total = list(terms)
    for s in sorted(range(1, len(terms)), key=lambda s: (-bin(s).count("1"), s)):
        sent = total[s].astype(BF)
        for bit, start, size in pieces_of(sent.shape[0], s):
            got = swap(sent[start : start + size], axis, bit).astype(F32)
            into = total[s ^ bit]
            if size == into.shape[0]:
                total[s ^ bit] = into + got
            else:
                rows = [into[:start], into[start : start + size] + got, into[start + size :]]
                total[s ^ bit] = jnp.concatenate([r for r in rows if r.shape[0]], axis=0)
    return total[0]


def exchange_columns(value, axis, index):
    size = lax.axis_size(axis)
    width = value.shape[1] // size
    out = [lax.dynamic_slice_in_dim(value, index * width, width, 1)]
    for s in range(1, size):
        part = lax.dynamic_slice_in_dim(value, (index ^ s) * width, width, 1)
        out.append(swap(part, axis, s))
    return out


def chain_sum(value, axis, position, length):
    half = length // 2

    def hop(value, moves):
        return lax.ppermute(value, axis, [(2 * a + c, 2 * b + c) for a, b in moves for c in (0, 1)])

    def add(a, b):
        return (a.astype(F32) + b.astype(F32)).astype(BF)

    total = value
    last = length - 1
    for step in range(half - 1):
        total = add(total, hop(total, [(step, step + 1), (last - step, last - step - 1)]))
    total = add(total, hop(total, [(half - 1, half), (half, half - 1)]))
    for step in reversed(range(half - 1)):
        got = hop(total, [(step + 1, step), (last - step - 1, last - step)])
        total = jnp.where((position == step) | (position == last - step), got, total)
    return total


def half_lanes(shape):
    return lax.broadcasted_iota(jnp.int32, shape, 1) % 128 < HEAD


def place(value, source, target):
    if source != target:
        value = pltpu.roll(value, HEAD, 1)
    low = half_lanes(value.shape)
    return jnp.where(low if target == 0 else ~low, value, 0.0)


def turn(value, cosine, sine):
    lane = lax.broadcasted_iota(jnp.int32, value.shape, 1) % HEAD
    partner = jnp.where(lane < HEAD // 2, pltpu.roll(value, 128 - HEAD // 2, 1), pltpu.roll(value, HEAD // 2, 1))
    return value * cosine + partner * sine


def rope_forward_body(width, kv_width, proj_ref, cos_ref, sin_ref, q_ref, kv_ref):
    cosine, sine = cos_ref[...], sin_ref[...]
    for at in range(0, width, 128):
        q_ref[:, at : at + 128] = (turn(proj_ref[:, at : at + 128], cosine, sine) * HEAD**-0.5).astype(BF)
    for at in range(0, kv_width, 128):
        kv_ref[:, at : at + 128] = turn(proj_ref[:, width + at : width + at + 128], cosine, sine).astype(BF)
    kv_ref[:, kv_width:] = proj_ref[:, width + kv_width :].astype(BF)


def rope_backward_body(width, kv_width, gq_ref, gkv_ref, cos_ref, sin_ref, out_ref):
    cosine, sine = cos_ref[...], -sin_ref[...]
    for at in range(0, width, 128):
        out_ref[:, at : at + 128] = turn(gq_ref[:, at : at + 128], cosine, sine).astype(BF)
    for at in range(0, kv_width, 128):
        out_ref[:, width + at : width + at + 128] = turn(gkv_ref[:, at : at + 128], cosine, sine).astype(BF)
    out_ref[:, width + kv_width :] = gkv_ref[:, kv_width:].astype(BF)


def whole(*arrays):
    return [pl.BlockSpec(a.shape, lambda *_: (0,) * a.ndim) for a in arrays]


def attention_forward_body(rows, per_kv, bounds_ref, q_ref, k_ref, v_ref, start_ref, out_ref, lse_ref):
    first, low_block, last_block = bounds_ref[0], bounds_ref[1], bounds_ref[2]
    row = first + lax.broadcasted_iota(jnp.int32, (rows, rows), 1)
    key_in_block = lax.broadcasted_iota(jnp.int32, (rows, rows), 0)
    start = start_ref[...]
    groups = [[(c, j, e) for c in range(2) for j in range(per_kv // 2) for e in range(2)]]
    for these in groups:
            heads = []
            for c, j, e in these:
                at = (c * (per_kv // 2) + j) * 128
                heads.append(place(q_ref[:, at : at + 128].astype(F32), e, c).astype(BF))

            def block(i, carry):
                kb = last_block - i
                rows_of = pl.ds(pl.multiple_of(kb * rows, rows), rows)
                k_block = k_ref[rows_of, :]
                v_block = v_ref[rows_of, :]
                key = key_in_block + kb * rows
                mask = (key <= row) & (key >= start)
                new = []
                scores = [jnp.where(mask, mm(k_block, h, 1, 1), NEG) for h in heads]
                for e, s in enumerate(scores):
                    top, total, mixed = carry[3 * e : 3 * e + 3]
                    raised = jnp.maximum(top, jnp.max(s, axis=0, keepdims=True))
                    fade = jnp.exp(top - raised)
                    p = jnp.exp(s - raised)
                    total = total * fade + jnp.sum(p, axis=0, keepdims=True)
                    new += [raised, total, mixed * fade + mm(v_block, p.astype(BF), 0, 0)]
                return tuple(new)

            begin = (jnp.full((1, rows), NEG, F32), jnp.zeros((1, rows), F32), jnp.zeros((128, rows), F32))
            carry = lax.fori_loop(0, last_block + 1 - low_block, block, begin * len(these))
            parts = {}
            for i, (c, j, e) in enumerate(these):
                index = c * per_kv + 2 * j + e
                top, total, mixed = carry[3 * i : 3 * i + 3]
                lse_ref[index : index + 1, :] = top + jnp.log(total)
                parts[c, j, e] = mixed[c * HEAD : (c + 1) * HEAD] / total
            for c, j, e in these:
                if e == 0:
                    at = (c * (per_kv // 2) + j) * 128
                    both = jnp.concatenate([parts[c, j, 0], parts[c, j, 1]], axis=0)
                    out_ref[:, at : at + 128] = jnp.transpose(both).astype(BF)


def attention_backward_body(
    rows, per_kv, bounds_ref, q_ref, o_ref, g_ref, k_ref, v_ref, lse_ref, start_ref, gq_ref, gk_ref, gv_ref
):
    first, low_block, last_block = bounds_ref[0], bounds_ref[1], bounds_ref[2]
    row = first + lax.broadcasted_iota(jnp.int32, (rows, rows), 1)
    key_in_block = lax.broadcasted_iota(jnp.int32, (rows, rows), 0)
    start = start_ref[...]
    gk_ref[...] = jnp.zeros(gk_ref.shape, F32)
    gv_ref[...] = jnp.zeros(gv_ref.shape, F32)
    groups = [[(c, j) for c in range(2) for j in range(per_kv // 2)]]
    for these in groups:
        info = []
        for c, j in these:
            at = (c * (per_kv // 2) + j) * 128
            q_pair = q_ref[:, at : at + 128].astype(F32)
            g_pair = g_ref[:, at : at + 128].astype(F32)
            product = jnp.transpose(g_pair * o_ref[:, at : at + 128].astype(F32))
            for e in range(2):
                index = c * per_kv + 2 * j + e
                info.append(
                    (
                        place(q_pair, e, c).astype(BF),
                        place(g_pair, e, c).astype(BF),
                        jnp.sum(product[e * HEAD : (e + 1) * HEAD], axis=0, keepdims=True),
                        lse_ref[index : index + 1, :],
                    )
                )

        def block(kb, carry):
            rows_of = pl.ds(pl.multiple_of(kb * rows, rows), rows)
            k_block = k_ref[rows_of, :]
            v_block = v_ref[rows_of, :]
            key = key_in_block + kb * rows
            mask = (key <= row) & (key >= start)
            new = []
            grad_k = gk_ref[rows_of, :]
            grad_v = gv_ref[rows_of, :]
            for (q_head, g_head, inner, logs), grad_q in zip(info, carry):
                s = jnp.where(mask, mm(k_block, q_head, 1, 1), NEG)
                p = jnp.exp(s - logs)
                grad_p = mm(v_block, g_head, 1, 1)
                grad_s = (p * (grad_p - inner)).astype(BF)
                grad_v = grad_v + mm(p.astype(BF), g_head, 1, 0)
                grad_k = grad_k + mm(grad_s, q_head, 1, 0)
                new.append(grad_q + mm(grad_s, k_block, 0, 0))
            gk_ref[rows_of, :] = grad_k
            gv_ref[rows_of, :] = grad_v
            return tuple(new)

        zero = jnp.zeros((rows, 128), F32)
        grads = lax.fori_loop(low_block, last_block + 1, block, (zero,) * len(info))
        for i, (c, j) in enumerate(these):
            at = (c * (per_kv // 2) + j) * 128
            total = place(grads[2 * i], c, 0) + place(grads[2 * i + 1], c, 1)
            gq_ref[:, at : at + 128] = total * HEAD**-0.5


def attention_forward(bounds, queries, keys_values, start):
    rows, width = queries.shape
    length, kv2 = keys_values.shape
    pairs = kv2 // 2 // 128
    wide = width // pairs
    per_kv = wide // (2 * HEAD)
    spec = pltpu.PrefetchScalarGridSpec(
        num_scalar_prefetch=1,
        grid=(pairs,),
        in_specs=[
            pl.BlockSpec((rows, wide), lambda i, b: (0, i)),
            pl.BlockSpec((length, 128), lambda i, b: (0, i)),
            pl.BlockSpec((length, 128), lambda i, b: (0, i + pairs)),
            pl.BlockSpec((1, rows), lambda i, b: (0, 0)),
        ],
        out_specs=[
            pl.BlockSpec((rows, wide), lambda i, b: (0, i)),
            pl.BlockSpec((2 * per_kv, rows), lambda i, b: (i, 0)),
        ],
    )
    return pl.pallas_call(
        functools.partial(attention_forward_body, rows, per_kv),
        grid_spec=spec,
        out_shape=[
            jax.ShapeDtypeStruct((rows, width), BF),
            jax.ShapeDtypeStruct((2 * per_kv * pairs, rows), F32),
        ],
        cost_estimate=pl.CostEstimate(
            flops=8 * rows * length * width, transcendentals=rows * length * width // HEAD, bytes_accessed=8 * rows * width
        ),
        name="attention_forward",
    )(bounds, queries, keys_values, keys_values, start[None])


def attention_backward(bounds, queries, attended, grad, keys_values, logs, start, base, count):
    rows, width = queries.shape
    length, kv2 = keys_values.shape
    pairs = kv2 // 2 // 128
    wide = width // pairs
    per_kv = wide // (2 * HEAD)
    row_block = pl.BlockSpec((rows, wide), lambda i, b: (0, i + base))
    spec = pltpu.PrefetchScalarGridSpec(
        num_scalar_prefetch=1,
        grid=(count,),
        in_specs=[
            row_block,
            row_block,
            row_block,
            pl.BlockSpec((length, 128), lambda i, b: (0, i + base)),
            pl.BlockSpec((length, 128), lambda i, b: (0, i + base + pairs)),
            pl.BlockSpec((2 * per_kv, rows), lambda i, b: (i + base, 0)),
            pl.BlockSpec((1, rows), lambda i, b: (0, 0)),
        ],
        out_specs=[
            pl.BlockSpec((rows, wide), lambda i, b: (0, i)),
            pl.BlockSpec((length, 128), lambda i, b: (0, i)),
            pl.BlockSpec((length, 128), lambda i, b: (0, i)),
        ],
    )
    return pl.pallas_call(
        functools.partial(attention_backward_body, rows, per_kv),
        grid_spec=spec,
        out_shape=[
            jax.ShapeDtypeStruct((rows, wide * count), F32),
            jax.ShapeDtypeStruct((length, 128 * count), F32),
            jax.ShapeDtypeStruct((length, 128 * count), F32),
        ],
        cost_estimate=pl.CostEstimate(
            flops=20 * rows * length * wide * count,
            transcendentals=rows * length * wide * count // HEAD,
            bytes_accessed=8 * rows * width,
        ),
        name="attention_backward",
    )(bounds, queries, attended, grad, keys_values, keys_values, logs, start[None])
class Chain:
    def __init__(self, axis, position, length):
        self.axis, self.position, self.length = axis, position, length
        self.queue, self.sums, self.done = [], {}, {}
        self.tick = 0
        self.token = self.last = ()

    def feed(self, chunk):
        if self.length != 4:
            self.done[len(self.queue)] = chain_sum(chunk, self.axis, self.position, self.length)
        self.queue.append(chunk)
        return len(self.queue) - 1

    def hop(self, value, moves):
        return lax.ppermute(
            value, self.axis, [(2 * a + c, 2 * b + c) for a, b in moves for c in (0, 1)]
        )

    def step(self, *guards):
        if self.length != 4:
            return
        t = self.tick
        self.tick += 1
        outer = (self.position == 0) | (self.position == 3)
        fresh = self.queue[t] if t < len(self.queue) else None
        across = self.sums.get(t - 1)
        final = self.sums.get((t - 2, 1))
        sent = [v for v in (fresh, across, final) if v is not None]
        if not sent:
            return
        held = lax.optimization_barrier((*sent, *self.token, *guards))
        sent = iter(held[: len(sent)])
        fresh = next(sent) if fresh is not None else None
        across = next(sent) if across is not None else None
        final = next(sent) if final is not None else None
        if fresh is None:
            outgoing = final
        elif final is None:
            outgoing = fresh
        else:
            columns = max(fresh.shape[1], final.shape[1])
            outgoing = jnp.where(outer, widen(fresh, columns), widen(final, columns))
        marks = []
        if outgoing is not None:
            got = self.hop(outgoing, [(0, 1), (1, 0), (2, 3), (3, 2)])
            marks.append(got)
            if fresh is not None:
                self.sums[t] = rounded_sum(fresh, got[:, : fresh.shape[1]])
            if final is not None:
                self.done[t - 2] = jnp.where(outer, got[:, : final.shape[1]], final)
        if across is not None:
            got = self.hop(across, [(0, 0), (1, 2), (2, 1), (3, 3)])
            self.sums[t - 1, 1] = rounded_sum(across, got)
            marks.append(got)
        self.last, self.token = self.token, tuple(marks)

    def hold(self, value):
        return after(value, *self.last) if self.last else value


def widen(value, columns):
    short = columns - value.shape[1]
    return jnp.pad(value, ((0, 0), (0, short))) if short else value


def after(value, *others):
    return lax.optimization_barrier((value, *others))[0]


def rounded_sum(a, b):
    return (a.astype(F32) + b.astype(F32)).astype(BF)


def place_rows_body(parity_ref, own_ref, other_ref, out_ref):
    own = pl.program_id(0) < pl.num_programs(0) // 2

    @pl.when(own)
    def _():
        out_ref[...] = own_ref[...].astype(F32)

    @pl.when(~own)
    def _():
        out_ref[...] = other_ref[...].astype(F32)


def place_pairs_body(parity_ref, own_a_ref, other_a_ref, own_b_ref, other_b_ref, out_ref):
    own = pl.program_id(0) < pl.num_programs(0) // 2

    @pl.when(own)
    def _():
        out_ref[:, 0, :] = own_a_ref[...].astype(F32)
        out_ref[:, 1, :] = own_b_ref[...].astype(F32)

    @pl.when(~own)
    def _():
        out_ref[:, 0, :] = other_a_ref[...].astype(F32)
        out_ref[:, 1, :] = other_b_ref[...].astype(F32)


def place_halves(parity, *halves):
    rows, width = halves[0].shape
    size = 64 if rows % 64 == 0 else rows
    if len(halves) == 2 and rows % 128 == 0:
        size = 128
    count = rows // size
    own = pl.BlockSpec((size, width), lambda i, p: (jnp.minimum(i, count - 1), 0))
    other = pl.BlockSpec((size, width), lambda i, p: (jnp.maximum(i - count, 0), 0))

    def spot(i, p):
        return jnp.where(i < count, p[0] * count + i, (1 - p[0]) * count + i - count)

    if len(halves) == 2:
        body, shape = place_rows_body, (2 * rows, width)
        out = pl.BlockSpec((size, width), lambda i, p: (spot(i, p), 0))
    else:
        body, shape = place_pairs_body, (2 * rows, 2, width)
        out = pl.BlockSpec((size, 2, width), lambda i, p: (spot(i, p), 0, 0))
    spec = pltpu.PrefetchScalarGridSpec(
        num_scalar_prefetch=1, grid=(2 * count,), in_specs=[own, other] * (len(halves) // 2), out_specs=out
    )
    return pl.pallas_call(
        body,
        grid_spec=spec,
        out_shape=jax.ShapeDtypeStruct(shape, F32),
        cost_estimate=pl.CostEstimate(
            flops=rows * width * 2, transcendentals=0, bytes_accessed=6 * rows * width * len(halves)
        ),
        name="place_halves",
    )(parity[None], *halves)


def shards(tokens, segments, positions, norm_in, w_qkv, w_out, norm_mid, w_in, w_down, cotangent):
    inputs = tokens[0]
    local_rows, width = inputs.shape
    qkv_cols = w_qkv.shape[1]
    kv_width = (qkv_cols - width) // 2
    group_size = lax.axis_size("group")
    group_index = lax.axis_index("group")
    replica_index = lax.axis_index("replica")
    parity = replica_index % 2
    position = replica_index // 2
    length = lax.axis_size("replica") // 2
    first_row = group_index * local_rows
    seq_ids = segments[0]
    seq_len = seq_ids.shape[0]

    def gather_weight(weight, *others):
        rows = weight.shape[0]
        half = rows // 2
        mine = lax.dynamic_slice_in_dim(weight, parity * half, half, 0)
        if others:
            mine = after(mine, *others)
        full = jnp.zeros((rows * group_size, weight.shape[1]), weight.dtype)
        blocks = gather_blocks(mine, "group")
        for s, block in enumerate(blocks):
            base = (group_index ^ s) * rows
            if s == 0:
                full = lax.dynamic_update_slice_in_dim(full, weight, base, 0)
                continue
            full = lax.dynamic_update_slice_in_dim(full, block, base + parity * half, 0)
            other = swap(block, "replica", 1)
            full = lax.dynamic_update_slice_in_dim(full, other, base + (1 - parity) * half, 0)
        return full, blocks[-1]

    def gather_rows(own):
        rows = own.shape[0]
        full = jnp.zeros((rows * group_size, own.shape[1]), own.dtype)
        for s, block in enumerate(gather_blocks(own, "group")):
            full = lax.dynamic_update_slice_in_dim(full, block, (group_index ^ s) * rows, 0)
        return full

    qkv_full, qkv_mark = gather_weight(w_qkv)
    gains = jnp.stack([norm_in, norm_mid])
    gain_full = jnp.zeros((2, width), BF)
    gain_full = lax.dynamic_update_slice_in_dim(gain_full, gains, group_index * norm_in.shape[0], 1)
    for s in range(1, group_size):
        gain_full = lax.dynamic_update_slice_in_dim(
            gain_full, swap(gains, "group", s), (group_index ^ s) * norm_in.shape[0], 1
        )
    gain_in_float = gain_full[0].astype(F32)
    gain_mid_float = gain_full[1].astype(F32)

    own_ids = lax.dynamic_slice_in_dim(seq_ids, first_row, local_rows)
    starts = jnp.sum((seq_ids[None, :] < own_ids[:, None]).astype(jnp.int32), axis=1)
    bounds = jnp.stack([first_row, starts[0] // local_rows, group_index]).astype(jnp.int32)
    cosine, sine = rope_tables(positions[0], HEAD)
    cosine = jnp.concatenate([cosine] * 4, axis=1)
    sine = jnp.concatenate([-sine, sine] * 2, axis=1)
    input_float = inputs.astype(F32)
    scale_in = rms_scale(input_float)
    unit_in = input_float * scale_in
    normed_in = (unit_in * gain_in_float).astype(BF)
    projected = mm(normed_in, qkv_full, 1, 0)
    queries, kv_own = pl.pallas_call(
        functools.partial(rope_forward_body, width, kv_width),
        in_specs=whole(projected, cosine, sine),
        out_specs=whole(inputs, inputs[:, : 2 * kv_width]),
        out_shape=[
            jax.ShapeDtypeStruct((local_rows, width), BF),
            jax.ShapeDtypeStruct((local_rows, 2 * kv_width), BF),
        ],
        name="rope_forward",
    )(projected, cosine, sine)
    kv_all = gather_rows(kv_own)
    out_full, _ = gather_weight(w_out, qkv_mark)
    grad_out = cotangent[0]
    grad_blocks = gather_blocks(after(grad_out, kv_all), "group")

    attended, logs = attention_forward(bounds, queries, kv_all, starts)
    middle = input_float + mm(attended, out_full, 1, 0)
    scale_mid = rms_scale(middle)
    unit_mid = middle * scale_mid
    normed_mid = (unit_mid * gain_mid_float).astype(BF)

    mlp_rows = jnp.concatenate(gather_blocks(normed_mid, "group"), axis=0)
    grad_rows = jnp.concatenate(grad_blocks, axis=0)
    grad_hidden = lax.optimization_barrier(mm(grad_rows, w_down, 1, 1))
    gate_up = jnp.einsum("td,nkd->tkn", mlp_rows, w_in, preferred_element_type=F32)
    normed_cols = exchange_columns(after(normed_in, mlp_rows), "group", group_index)
    attended_cols = exchange_columns(after(attended, *normed_cols[1:]), "group", group_index)
    gate, up = gate_up[:, 0], gate_up[:, 1]
    sigma = jax.nn.sigmoid(gate)
    hidden = (gate * sigma * up).astype(BF)
    grad_gate = (grad_hidden * up * (sigma * (1.0 + gate * (1.0 - sigma)))).astype(BF)
    grad_up = (grad_hidden * gate * sigma).astype(BF)

    chain = Chain("replica", position, length)

    def other_half(left, right):
        half = left.shape[1] // 2
        term = mm(lax.dynamic_slice_in_dim(left, (1 - parity) * half, half, 1), right, 0, 0).astype(BF)
        return swap(term, "replica", 1), term

    def own_half(left, right, got):
        half = left.shape[1] // 2
        own = mm(lax.dynamic_slice_in_dim(left, parity * half, half, 1), right, 0, 0)
        return (own + got.astype(F32)).astype(BF)

    def enqueue(own, rows):
        rows = min(rows, own.shape[0])
        return [chain.feed(own[i : i + rows]) for i in range(0, own.shape[0], rows)]

    def collect(numbers, axis=0):
        own = jnp.concatenate([chain.done[n] for n in numbers], axis=axis)
        return own, swap(own, "replica", 1)

    def blocks_of(value):
        return [value[s * local_rows : (s + 1) * local_rows] for s in range(group_size)]

    down_got, _ = other_half(hidden, grad_rows)
    down_numbers = enqueue(own_half(hidden, grad_rows, down_got), CHUNK)

    chain.step()
    grad_gate_up = jnp.stack([grad_gate, grad_up], axis=1)
    back_term = jnp.einsum("tkn,nkd->td", grad_gate_up, w_in, preferred_element_type=F32)
    grad_normed = scatter_sum(blocks_of(back_term), "group")

    chain.step(back_term)
    gate_got, gate_term = other_half(chain.hold(grad_gate), mlp_rows)
    gate_own = own_half(after(grad_gate, gate_term), mlp_rows, gate_got)
    gate_numbers = enqueue(gate_own, CHUNK)

    chain.step(gate_own)
    grad_mid_norm, gain_mid_term = norm_backward(
        chain.hold(grad_normed), unit_mid, scale_mid, gain_mid_float
    )
    grad_middle = grad_out.astype(F32) + grad_mid_norm
    grad_branch = grad_middle.astype(BF)
    grad_attended = mm(grad_branch, out_full, 1, 1).astype(BF)
    branch_blocks = gather_blocks(grad_branch, "group")

    pairs = kv_width // 128
    parts = 2 if pairs % 2 == 0 else 1
    grads = []
    guard = grad_attended
    for i in range(parts):
        chain.step(guard)
        grads.append(
            attention_backward(
                bounds,
                queries,
                attended,
                chain.hold(grad_attended),
                kv_all,
                logs,
                starts,
                i * (pairs // parts),
                pairs // parts,
            )
        )
        guard = grads[-1][0]
    grad_query = jnp.concatenate([g[0] for g in grads], axis=1)
    kv_parts = [g[1] for g in grads] + [g[2] for g in grads]
    kv_terms = [
        jnp.concatenate(
            [
                lax.dynamic_slice_in_dim(part, (group_index ^ s) * local_rows, local_rows, 0)
                for part in kv_parts
            ],
            axis=1,
        ).astype(BF if s else F32)
        for s in range(group_size)
    ]
    kv_terms = [kv_terms[0]] + [after(v, branch_blocks[-1]) for v in kv_terms[1:]]
    kv_grad = scatter_sum(kv_terms, "group")

    chain.step(*kv_terms)
    up_got, up_term = other_half(chain.hold(grad_up), mlp_rows)
    chain.step(up_term)
    up_own = own_half(after(chain.hold(grad_up), up_term), mlp_rows, up_got)
    up_numbers = enqueue(up_own, CHUNK)
    grad_projected = pl.pallas_call(
        functools.partial(rope_backward_body, width, kv_width),
        in_specs=whole(grad_query, kv_grad, cosine, sine),
        out_specs=whole(projected)[0],
        out_shape=jax.ShapeDtypeStruct((local_rows, qkv_cols), BF),
        name="rope_backward",
    )(grad_query, kv_grad, cosine, sine)
    proj_blocks = gather_blocks(grad_projected, "group")

    chain.step(up_own, grad_projected)
    feed_term = mm(chain.hold(hidden), w_down, 1, 0)
    feed_sum = scatter_sum(blocks_of(after(feed_term, proj_blocks[-1])), "group")
    output = (middle + feed_sum).astype(BF)

    chain.step(feed_term)
    grad_normed_in = mm(chain.hold(grad_projected), qkv_full, 1, 1)
    grad_in_norm, gain_in_term = norm_backward(grad_normed_in, unit_in, scale_in, gain_in_float)
    grad_input = (grad_middle + grad_in_norm).astype(BF)

    chain.step(grad_input)
    attended_rows = chain.hold(jnp.concatenate(attended_cols, axis=0))
    branch_rows = jnp.concatenate(branch_blocks, axis=0)
    out_got, out_term = other_half(attended_rows, branch_rows)
    out_own = own_half(attended_rows, branch_rows, out_got)
    out_numbers = enqueue(out_own, CHUNK)

    chain.step(out_own)
    down_own, down_other = collect(down_numbers)
    down_sum = place_halves(parity, chain.hold(down_own), down_other)

    chain.step(down_sum)
    proj_rows = chain.hold(jnp.concatenate(proj_blocks, axis=0))
    normed_rows = jnp.concatenate(normed_cols, axis=0)
    qkv_got, qkv_term = other_half(normed_rows, proj_rows)
    qkv_own = own_half(normed_rows, proj_rows, qkv_got)
    qkv_numbers = [chain.feed(qkv_own[:, :width]), chain.feed(qkv_own[:, width:])]

    chain.step(qkv_own)
    while chain.length == 4 and len(chain.done) < max(up_numbers) + 1:
        chain.step()
    gate_own, gate_other = collect(gate_numbers)
    up_own, up_other = collect(up_numbers)
    in_sum = place_halves(parity, gate_own, gate_other, chain.hold(up_own), up_other)
    chain.step()
    while chain.length == 4 and len(chain.done) < len(chain.queue):
        chain.step()
    out_sum = place_halves(parity, *collect(out_numbers))
    qkv_sum = place_halves(parity, *collect(qkv_numbers, 1))

    gain_terms = jnp.stack([gain_in_term, gain_mid_term])
    parts = exchange_columns(gain_terms, "group", group_index)
    gain_sum = sum(parts[1:], parts[0])
    for bit in range((lax.axis_size("replica") - 1).bit_length()):
        gain_sum = gain_sum + swap(gain_sum, "replica", 1 << bit)
    return (
        output[None],
        grad_input[None],
        gain_sum[0],
        qkv_sum,
        out_sum,
        gain_sum[1],
        in_sum,
        down_sum,
    )


def solution(mesh):
    return jax.shard_map(
        shards,
        mesh=mesh,
        in_specs=(
            P("replica", "group", None),
            P("replica", None),
            P("replica", "group"),
            P("group"),
            P("group", None),
            P("group", None),
            P("group"),
            P("group", None, None),
            P("group", None),
            P("replica", "group", None),
        ),
        out_specs=(
            P("replica", "group", None),
            P("replica", "group", None),
            P("group"),
            P("group", None),
            P("group", None),
            P("group"),
            P("group", None, None),
            P("group", None),
        ),
        check_vma=False,
    )
```

```python
import functools
import math

import jax
import jax.numpy as jnp
from jax import lax
from jax.experimental import pallas as pl
from jax.experimental.pallas import tpu as pltpu
from jax.sharding import PartitionSpec as P

HEAD = 64
EPS = 1e-05
ROPE_BASE = 500000.0
ROPE_FACTOR = 32.0
LOW_FACTOR = 1.0
HIGH_FACTOR = 4.0
OLD_CONTEXT = 8192.0
BF = jnp.bfloat16
F32 = jnp.float32
NEG = -1e30

CHUNK = 256


def rope_frequency(head_size):
    half = head_size // 2
    exponent = jnp.arange(half).astype(jnp.float32) * (2.0 / head_size)
    frequency = jnp.power(jnp.float32(ROPE_BASE), -exponent)
    wavelength = 2.0 * math.pi / frequency
    smooth = (OLD_CONTEXT / wavelength - LOW_FACTOR) / (HIGH_FACTOR - LOW_FACTOR)
    blended = (1.0 - smooth) * frequency / ROPE_FACTOR + smooth * frequency
    slow = jnp.where(wavelength > OLD_CONTEXT / LOW_FACTOR, frequency / ROPE_FACTOR, blended)
    return jnp.where(wavelength < OLD_CONTEXT / HIGH_FACTOR, frequency, slow)


def rope_tables(position, head_size):
    frequency = rope_frequency(head_size)
    angle = position.astype(jnp.float32)[:, None] * frequency[None, :]
    return (jnp.cos(angle), jnp.sin(angle))


def rms_scale(values):
    return lax.rsqrt(jnp.mean(values * values, axis=-1, keepdims=True) + EPS)


def norm_backward(grad_normed, unit, scale, gain):
    grad_unit = grad_normed * gain
    grad_input = scale * (grad_unit - unit * jnp.mean(grad_unit * unit, axis=-1, keepdims=True))
    return (grad_input, jnp.sum(grad_normed * unit, axis=0))


def mm(a, b, ca, cb):
    return lax.dot_general(a, b, (((ca,), (cb,)), ((), ())), preferred_element_type=F32)


def swap(value, axis, mask):
    return lax.ppermute(value, axis, [(i, i ^ mask) for i in range(lax.axis_size(axis))])


def bit_list(number):
    return [1 << b for b in range(number.bit_length()) if number >> b & 1]


def pieces_of(rows, number):
    bits = bit_list(number)
    while rows % (16 * len(bits)):
        bits = bits[:-1]
    step = rows // len(bits)
    return [(bit, i * step, step) for i, bit in enumerate(bits)]


def as_list(values):
    return list(values) if isinstance(values, (tuple, list)) else [values]


class Order:
    def __init__(self):
        self.marked = ()

    def hold(self, *values):
        held = lax.optimization_barrier((*values, *self.marked))[: len(values)] if self.marked else values
        return held[0] if len(held) == 1 else held

    def mark(self, *values):
        self.marked = values


class Gather:
    def __init__(self, own, axis):
        self.axis, self.size = axis, lax.axis_size(axis)
        self.rows = own.shape[0]
        self.blocks = {0: own}
        for s in range(1, self.size):
            if len(bit_list(s)) == 1:
                self.blocks[s] = swap(own, axis, s)

    def relay(self, hold=lambda *v: v):
        numbers = sorted(self.blocks)[1:]
        held = hold(*[self.blocks[s] for s in numbers]) if numbers else ()
        if len(numbers) == 1:
            held = (held[0] if isinstance(held, tuple) else held,)
        self.blocks.update(zip(numbers, held))
        for s in range(1, self.size):
            if s not in self.blocks:
                parts = [
                    swap(self.blocks[s ^ bit][start : start + size], self.axis, bit)
                    for bit, start, size in pieces_of(self.rows, s)
                ]
                self.blocks[s] = parts[0] if len(parts) == 1 else jnp.concatenate(parts, axis=0)
        return [self.blocks[s] for s in range(self.size)]


def gather_blocks(own, axis):
    return Gather(own, axis).relay()


class Scatter:
    def __init__(self, terms, axis):
        self.total, self.axis = list(terms), axis
        self.level = max(len(bit_list(s)) for s in range(len(terms)))

    def send(self):
        self.flying = []
        for s in range(1, len(self.total)):
            if len(bit_list(s)) == self.level:
                sent = self.total[s].astype(BF)
                for bit, start, size in pieces_of(sent.shape[0], s):
                    self.flying.append((s ^ bit, start, size, swap(sent[start : start + size], self.axis, bit)))
        self.level -= 1

    def receive(self, hold=lambda *v: v):
        got = hold(*[f[3] for f in self.flying])
        got = got if isinstance(got, (tuple, list)) else (got,)
        for (s, start, size, _), value in zip(self.flying, got):
            into, value = self.total[s], value.astype(F32)
            if size == into.shape[0]:
                self.total[s] = into + value
            else:
                rows = [into[:start], into[start : start + size] + value, into[start + size :]]
                self.total[s] = jnp.concatenate([r for r in rows if r.shape[0]], axis=0)
        return self.total[0]

    def relay(self, hold=lambda *v: v):
        while self.level:
            self.receive(hold)
            self.send()


def exchange_columns(value, axis, index):
    size = lax.axis_size(axis)
    width = value.shape[1] // size
    out = [lax.dynamic_slice_in_dim(value, index * width, width, 1)]
    for s in range(1, size):
        part = lax.dynamic_slice_in_dim(value, (index ^ s) * width, width, 1)
        out.append(swap(part, axis, s))
    return out


def chain_sum(value, axis, position, length):
    half = length // 2

    def hop(value, moves):
        return lax.ppermute(value, axis, [(2 * a + c, 2 * b + c) for a, b in moves for c in (0, 1)])

    def add(a, b):
        return (a.astype(F32) + b.astype(F32)).astype(BF)

    total = value
    last = length - 1
    for step in range(half - 1):
        total = add(total, hop(total, [(step, step + 1), (last - step, last - step - 1)]))
    total = add(total, hop(total, [(half - 1, half), (half, half - 1)]))
    for step in reversed(range(half - 1)):
        got = hop(total, [(step + 1, step), (last - step - 1, last - step)])
        total = jnp.where((position == step) | (position == last - step), got, total)
    return total


def half_lanes(shape):
    return lax.broadcasted_iota(jnp.int32, shape, 1) % 128 < HEAD


def place(value, source, target):
    if source != target:
        value = pltpu.roll(value, HEAD, 1)
    low = half_lanes(value.shape)
    return jnp.where(low if target == 0 else ~low, value, 0.0)


def turn(value, cosine, sine):
    lane = lax.broadcasted_iota(jnp.int32, value.shape, 1) % HEAD
    partner = jnp.where(lane < HEAD // 2, pltpu.roll(value, 128 - HEAD // 2, 1), pltpu.roll(value, HEAD // 2, 1))
    return value * cosine + partner * sine


def rope_forward_body(width, kv_width, proj_ref, cos_ref, sin_ref, q_ref, kv_ref):
    cosine, sine = cos_ref[...], sin_ref[...]
    for at in range(0, width, 128):
        q_ref[:, at : at + 128] = (turn(proj_ref[:, at : at + 128], cosine, sine) * HEAD**-0.5).astype(BF)
    for at in range(0, kv_width, 128):
        kv_ref[:, at : at + 128] = turn(proj_ref[:, width + at : width + at + 128], cosine, sine).astype(BF)
    kv_ref[:, kv_width:] = proj_ref[:, width + kv_width :].astype(BF)


def rope_backward_body(width, kv_width, gq_ref, gkv_ref, cos_ref, sin_ref, out_ref):
    cosine, sine = cos_ref[...], -sin_ref[...]
    for at in range(0, width, 128):
        out_ref[:, at : at + 128] = turn(gq_ref[:, at : at + 128], cosine, sine).astype(BF)
    for at in range(0, kv_width, 128):
        out_ref[:, width + at : width + at + 128] = turn(gkv_ref[:, at : at + 128], cosine, sine).astype(BF)
    out_ref[:, width + kv_width :] = gkv_ref[:, kv_width:].astype(BF)


def whole(*arrays):
    return [pl.BlockSpec(a.shape, lambda *_: (0,) * a.ndim) for a in arrays]


def attention_forward_body(rows, per_kv, bounds_ref, q_ref, k_ref, v_ref, start_ref, out_ref, lse_ref):
    first, low_block, last_block = bounds_ref[0], bounds_ref[1], bounds_ref[2]
    row = first + lax.broadcasted_iota(jnp.int32, (rows, rows), 1)
    key_in_block = lax.broadcasted_iota(jnp.int32, (rows, rows), 0)
    start = start_ref[...]
    groups = [[(c, j, e) for c in range(2) for j in range(per_kv // 2) for e in range(2)]]
    for these in groups:
            heads = []
            for c, j, e in these:
                at = (c * (per_kv // 2) + j) * 128
                heads.append(place(q_ref[:, at : at + 128].astype(F32), e, c).astype(BF))

            def block(i, carry):
                kb = last_block - i
                rows_of = pl.ds(pl.multiple_of(kb * rows, rows), rows)
                k_block = k_ref[rows_of, :]
                v_block = v_ref[rows_of, :]
                key = key_in_block + kb * rows
                mask = (key <= row) & (key >= start)
                new = []
                scores = [jnp.where(mask, mm(k_block, h, 1, 1), NEG) for h in heads]
                for e, s in enumerate(scores):
                    top, total, mixed = carry[3 * e : 3 * e + 3]
                    raised = jnp.maximum(top, jnp.max(s, axis=0, keepdims=True))
                    fade = jnp.exp(top - raised)
                    p = jnp.exp(s - raised)
                    total = total * fade + jnp.sum(p, axis=0, keepdims=True)
                    new += [raised, total, mixed * fade + mm(v_block, p.astype(BF), 0, 0)]
                return tuple(new)

            begin = (jnp.full((1, rows), NEG, F32), jnp.zeros((1, rows), F32), jnp.zeros((128, rows), F32))
            carry = lax.fori_loop(0, last_block + 1 - low_block, block, begin * len(these))
            parts = {}
            for i, (c, j, e) in enumerate(these):
                index = c * per_kv + 2 * j + e
                top, total, mixed = carry[3 * i : 3 * i + 3]
                lse_ref[index : index + 1, :] = top + jnp.log(total)
                parts[c, j, e] = mixed[c * HEAD : (c + 1) * HEAD] / total
            for c, j, e in these:
                if e == 0:
                    at = (c * (per_kv // 2) + j) * 128
                    both = jnp.concatenate([parts[c, j, 0], parts[c, j, 1]], axis=0)
                    out_ref[:, at : at + 128] = jnp.transpose(both).astype(BF)


def attention_backward_body(
    rows, per_kv, bounds_ref, q_ref, o_ref, g_ref, k_ref, v_ref, lse_ref, start_ref, gq_ref, gk_ref, gv_ref
):
    first, low_block, last_block = bounds_ref[0], bounds_ref[1], bounds_ref[2]
    row = first + lax.broadcasted_iota(jnp.int32, (rows, rows), 1)
    key_in_block = lax.broadcasted_iota(jnp.int32, (rows, rows), 0)
    start = start_ref[...]
    gk_ref[...] = jnp.zeros(gk_ref.shape, F32)
    gv_ref[...] = jnp.zeros(gv_ref.shape, F32)
    groups = [[(c, j) for c in range(2) for j in range(per_kv // 2)]]
    for these in groups:
        info = []
        for c, j in these:
            at = (c * (per_kv // 2) + j) * 128
            q_pair = q_ref[:, at : at + 128].astype(F32)
            g_pair = g_ref[:, at : at + 128].astype(F32)
            product = jnp.transpose(g_pair * o_ref[:, at : at + 128].astype(F32))
            for e in range(2):
                index = c * per_kv + 2 * j + e
                info.append(
                    (
                        place(q_pair, e, c).astype(BF),
                        place(g_pair, e, c).astype(BF),
                        jnp.sum(product[e * HEAD : (e + 1) * HEAD], axis=0, keepdims=True),
                        lse_ref[index : index + 1, :],
                    )
                )

        def block(kb, carry):
            rows_of = pl.ds(pl.multiple_of(kb * rows, rows), rows)
            k_block = k_ref[rows_of, :]
            v_block = v_ref[rows_of, :]
            key = key_in_block + kb * rows
            mask = (key <= row) & (key >= start)
            new = []
            grad_k = gk_ref[rows_of, :]
            grad_v = gv_ref[rows_of, :]
            for (q_head, g_head, inner, logs), grad_q in zip(info, carry):
                s = jnp.where(mask, mm(k_block, q_head, 1, 1), NEG)
                p = jnp.exp(s - logs)
                grad_p = mm(v_block, g_head, 1, 1)
                grad_s = (p * (grad_p - inner)).astype(BF)
                grad_v = grad_v + mm(p.astype(BF), g_head, 1, 0)
                grad_k = grad_k + mm(grad_s, q_head, 1, 0)
                new.append(grad_q + mm(grad_s, k_block, 0, 0))
            gk_ref[rows_of, :] = grad_k
            gv_ref[rows_of, :] = grad_v
            return tuple(new)

        zero = jnp.zeros((rows, 128), F32)
        grads = lax.fori_loop(low_block, last_block + 1, block, (zero,) * len(info))
        for i, (c, j) in enumerate(these):
            at = (c * (per_kv // 2) + j) * 128
            total = place(grads[2 * i], c, 0) + place(grads[2 * i + 1], c, 1)
            gq_ref[:, at : at + 128] = total * HEAD**-0.5


def attention_forward(bounds, queries, keys_values, start):
    rows, width = queries.shape
    length, kv2 = keys_values.shape
    pairs = kv2 // 2 // 128
    wide = width // pairs
    per_kv = wide // (2 * HEAD)
    spec = pltpu.PrefetchScalarGridSpec(
        num_scalar_prefetch=1,
        grid=(pairs,),
        in_specs=[
            pl.BlockSpec((rows, wide), lambda i, b: (0, i)),
            pl.BlockSpec((length, 128), lambda i, b: (0, i)),
            pl.BlockSpec((length, 128), lambda i, b: (0, i + pairs)),
            pl.BlockSpec((1, rows), lambda i, b: (0, 0)),
        ],
        out_specs=[
            pl.BlockSpec((rows, wide), lambda i, b: (0, i)),
            pl.BlockSpec((2 * per_kv, rows), lambda i, b: (i, 0)),
        ],
    )
    return pl.pallas_call(
        functools.partial(attention_forward_body, rows, per_kv),
        grid_spec=spec,
        out_shape=[
            jax.ShapeDtypeStruct((rows, width), BF),
            jax.ShapeDtypeStruct((2 * per_kv * pairs, rows), F32),
        ],
        cost_estimate=pl.CostEstimate(
            flops=8 * rows * length * width, transcendentals=rows * length * width // HEAD, bytes_accessed=8 * rows * width
        ),
        name="attention_forward",
    )(bounds, queries, keys_values, keys_values, start[None])


def attention_backward(bounds, queries, attended, grad, keys_values, logs, start, base, count):
    rows, width = queries.shape
    length, kv2 = keys_values.shape
    pairs = kv2 // 2 // 128
    wide = width // pairs
    per_kv = wide // (2 * HEAD)
    row_block = pl.BlockSpec((rows, wide), lambda i, b: (0, i + base))
    spec = pltpu.PrefetchScalarGridSpec(
        num_scalar_prefetch=1,
        grid=(count,),
        in_specs=[
            row_block,
            row_block,
            row_block,
            pl.BlockSpec((length, 128), lambda i, b: (0, i + base)),
            pl.BlockSpec((length, 128), lambda i, b: (0, i + base + pairs)),
            pl.BlockSpec((2 * per_kv, rows), lambda i, b: (i + base, 0)),
            pl.BlockSpec((1, rows), lambda i, b: (0, 0)),
        ],
        out_specs=[
            pl.BlockSpec((rows, wide), lambda i, b: (0, i)),
            pl.BlockSpec((length, 128), lambda i, b: (0, i)),
            pl.BlockSpec((length, 128), lambda i, b: (0, i)),
        ],
    )
    return pl.pallas_call(
        functools.partial(attention_backward_body, rows, per_kv),
        grid_spec=spec,
        out_shape=[
            jax.ShapeDtypeStruct((rows, wide * count), F32),
            jax.ShapeDtypeStruct((length, 128 * count), F32),
            jax.ShapeDtypeStruct((length, 128 * count), F32),
        ],
        cost_estimate=pl.CostEstimate(
            flops=20 * rows * length * wide * count,
            transcendentals=rows * length * wide * count // HEAD,
            bytes_accessed=8 * rows * width,
        ),
        name="attention_backward",
    )(bounds, queries, attended, grad, keys_values, keys_values, logs, start[None])
class Chain:
    def __init__(self, axis, position, length):
        self.axis, self.position, self.length = axis, position, length
        self.queue, self.sums, self.done = [], {}, {}
        self.tick = 0
        self.flying = None

    def feed(self, chunk):
        if self.length != 4:
            self.done[len(self.queue)] = chain_sum(chunk, self.axis, self.position, self.length)
        self.queue.append(chunk)
        return len(self.queue) - 1

    def hop(self, value, moves, idle=()):
        pairs = [(2 * a + c, 2 * b + c) for a, b in moves for c in (0, 1)]
        return lax.ppermute(value, self.axis, pairs + [(2 * a + c, 2 * a + 1 - c) for a in idle for c in (0, 1)])

    def start(self, order):
        t = self.tick
        outer = (self.position == 0) | (self.position == 3)
        fresh = self.queue[t] if t < len(self.queue) else None
        across = self.sums.get(t - 1)
        final = self.sums.get((t - 2, 1))
        self.flying = None
        if self.length != 4 or (fresh is None and across is None and final is None):
            return
        if fresh is None:
            outgoing = final
        elif final is None:
            outgoing = fresh
        else:
            shape = tuple(map(max, zip(fresh.shape, final.shape)))
            outgoing = jnp.where(outer, widen(fresh, shape), widen(final, shape))
        sent = [v for v in (outgoing, across) if v is not None]
        held = order.hold(*sent)
        held = list(held) if len(sent) > 1 else [held]
        got = []
        if outgoing is not None:
            got.append(self.hop(held.pop(0), [(0, 1), (1, 0), (2, 3), (3, 2)]))
        if across is not None:
            got.append(self.hop(held.pop(0), [(1, 2), (2, 1)], (0, 3)))
        self.flying = (outer, fresh, across, final, got)

    def fold(self, order):
        t = self.tick
        self.tick += 1
        if self.flying is None:
            return
        outer, fresh, across, final, got = self.flying
        held = order.hold(*got)
        held = list(held) if len(got) > 1 else [held]
        marks = []
        if fresh is not None or final is not None:
            value = held.pop(0)
            if fresh is not None:
                self.sums[t] = rounded_sum(fresh, cut(value, fresh.shape))
                marks.append(self.sums[t])
            if final is not None:
                self.done[t - 2] = jnp.where(outer, cut(value, final.shape), final)
        if across is not None:
            self.sums[t - 1, 1] = rounded_sum(across, held.pop(0))
            marks.append(self.sums[t - 1, 1])
        order.mark(*(marks or held or got))


def widen(value, shape):
    pads = [(0, want - have) for want, have in zip(shape, value.shape)]
    return jnp.pad(value, pads) if any(p[1] for p in pads) else value


def cut(value, shape):
    return value[: shape[0], : shape[1]]


def after(value, *others):
    return lax.optimization_barrier((value, *others))[0]


def rounded_sum(a, b):
    return (a.astype(F32) + b.astype(F32)).astype(BF)


def place_rows_body(parity_ref, own_ref, other_ref, out_ref):
    own = pl.program_id(0) < pl.num_programs(0) // 2

    @pl.when(own)
    def _():
        out_ref[...] = own_ref[...].astype(F32)

    @pl.when(~own)
    def _():
        out_ref[...] = other_ref[...].astype(F32)


def place_pairs_body(parity_ref, own_a_ref, other_a_ref, own_b_ref, other_b_ref, out_ref):
    own = pl.program_id(0) < pl.num_programs(0) // 2

    @pl.when(own)
    def _():
        out_ref[:, 0, :] = own_a_ref[...].astype(F32)
        out_ref[:, 1, :] = own_b_ref[...].astype(F32)

    @pl.when(~own)
    def _():
        out_ref[:, 0, :] = other_a_ref[...].astype(F32)
        out_ref[:, 1, :] = other_b_ref[...].astype(F32)


def place_halves(parity, *halves):
    rows, width = halves[0].shape
    size = 64 if rows % 64 == 0 else rows
    if len(halves) == 2 and rows % 128 == 0:
        size = 128
    count = rows // size
    own = pl.BlockSpec((size, width), lambda i, p: (jnp.minimum(i, count - 1), 0))
    other = pl.BlockSpec((size, width), lambda i, p: (jnp.maximum(i - count, 0), 0))

    def spot(i, p):
        return jnp.where(i < count, p[0] * count + i, (1 - p[0]) * count + i - count)

    if len(halves) == 2:
        body, shape = place_rows_body, (2 * rows, width)
        out = pl.BlockSpec((size, width), lambda i, p: (spot(i, p), 0))
    else:
        body, shape = place_pairs_body, (2 * rows, 2, width)
        out = pl.BlockSpec((size, 2, width), lambda i, p: (spot(i, p), 0, 0))
    spec = pltpu.PrefetchScalarGridSpec(
        num_scalar_prefetch=1, grid=(2 * count,), in_specs=[own, other] * (len(halves) // 2), out_specs=out
    )
    return pl.pallas_call(
        body,
        grid_spec=spec,
        out_shape=jax.ShapeDtypeStruct(shape, F32),
        cost_estimate=pl.CostEstimate(
            flops=rows * width * 2, transcendentals=0, bytes_accessed=6 * rows * width * len(halves)
        ),
        name="place_halves",
    )(parity[None], *halves)


def shards(tokens, segments, positions, norm_in, w_qkv, w_out, norm_mid, w_in, w_down, cotangent):
    inputs = tokens[0]
    local_rows, width = inputs.shape
    qkv_cols = w_qkv.shape[1]
    kv_width = (qkv_cols - width) // 2
    group_size = lax.axis_size("group")
    group_index = lax.axis_index("group")
    replica_index = lax.axis_index("replica")
    parity = replica_index % 2
    position = replica_index // 2
    length = lax.axis_size("replica") // 2
    first_row = group_index * local_rows
    seq_ids = segments[0]
    seq_len = seq_ids.shape[0]

    def gather_weight(weight, *others):
        rows = weight.shape[0]
        half = rows // 2
        mine = lax.dynamic_slice_in_dim(weight, parity * half, half, 0)
        if others:
            mine = after(mine, *others)
        full = jnp.zeros((rows * group_size, weight.shape[1]), weight.dtype)
        blocks = gather_blocks(mine, "group")
        for s, block in enumerate(blocks):
            base = (group_index ^ s) * rows
            if s == 0:
                full = lax.dynamic_update_slice_in_dim(full, weight, base, 0)
                continue
            full = lax.dynamic_update_slice_in_dim(full, block, base + parity * half, 0)
            other = swap(block, "replica", 1)
            full = lax.dynamic_update_slice_in_dim(full, other, base + (1 - parity) * half, 0)
        return full, blocks[-1]

    def gather_rows(own):
        rows = own.shape[0]
        full = jnp.zeros((rows * group_size, own.shape[1]), own.dtype)
        for s, block in enumerate(gather_blocks(own, "group")):
            full = lax.dynamic_update_slice_in_dim(full, block, (group_index ^ s) * rows, 0)
        return full

    qkv_full, qkv_mark = gather_weight(w_qkv)
    gains = jnp.stack([norm_in, norm_mid])
    gain_full = jnp.zeros((2, width), BF)
    gain_full = lax.dynamic_update_slice_in_dim(gain_full, gains, group_index * norm_in.shape[0], 1)
    for s in range(1, group_size):
        gain_full = lax.dynamic_update_slice_in_dim(
            gain_full, swap(gains, "group", s), (group_index ^ s) * norm_in.shape[0], 1
        )
    gain_in_float = gain_full[0].astype(F32)
    gain_mid_float = gain_full[1].astype(F32)

    own_ids = lax.dynamic_slice_in_dim(seq_ids, first_row, local_rows)
    starts = jnp.sum((seq_ids[None, :] < own_ids[:, None]).astype(jnp.int32), axis=1)
    bounds = jnp.stack([first_row, starts[0] // local_rows, group_index]).astype(jnp.int32)
    cosine, sine = rope_tables(positions[0], HEAD)
    cosine = jnp.concatenate([cosine] * 4, axis=1)
    sine = jnp.concatenate([-sine, sine] * 2, axis=1)
    input_float = inputs.astype(F32)
    scale_in = rms_scale(input_float)
    unit_in = input_float * scale_in
    normed_in = (unit_in * gain_in_float).astype(BF)
    projected = mm(normed_in, qkv_full, 1, 0)
    queries, kv_own = pl.pallas_call(
        functools.partial(rope_forward_body, width, kv_width),
        in_specs=whole(projected, cosine, sine),
        out_specs=whole(inputs, inputs[:, : 2 * kv_width]),
        out_shape=[
            jax.ShapeDtypeStruct((local_rows, width), BF),
            jax.ShapeDtypeStruct((local_rows, 2 * kv_width), BF),
        ],
        name="rope_forward",
    )(projected, cosine, sine)
    kv_all = gather_rows(kv_own)
    out_full, _ = gather_weight(w_out, qkv_mark)
    grad_out = cotangent[0]
    grad_blocks = gather_blocks(after(grad_out, kv_all), "group")

    attended, logs = attention_forward(bounds, queries, kv_all, starts)
    middle = input_float + mm(attended, out_full, 1, 0)
    scale_mid = rms_scale(middle)
    unit_mid = middle * scale_mid
    normed_mid = (unit_mid * gain_mid_float).astype(BF)

    mlp_rows = jnp.concatenate(gather_blocks(normed_mid, "group"), axis=0)
    grad_rows = jnp.concatenate(grad_blocks, axis=0)
    grad_hidden = lax.optimization_barrier(mm(grad_rows, w_down, 1, 1))
    gate_up = jnp.einsum("td,nkd->tkn", mlp_rows, w_in, preferred_element_type=F32)
    normed_cols = exchange_columns(after(normed_in, mlp_rows), "group", group_index)
    gate, up = gate_up[:, 0], gate_up[:, 1]
    sigma = jax.nn.sigmoid(gate)
    hidden = (gate * sigma * up).astype(BF)
    grad_gate = (grad_hidden * up * (sigma * (1.0 + gate * (1.0 - sigma)))).astype(BF)
    grad_up = (grad_hidden * gate * sigma).astype(BF)

    order = Order()
    chain = Chain("replica", position, length)

    def other_half(left, right):
        half = left.shape[1] // 2
        left = order.hold(left)
        term = mm(lax.dynamic_slice_in_dim(left, (1 - parity) * half, half, 1), right, 0, 0).astype(BF)
        order.mark(term)
        return swap(term, "replica", 1)

    def own_half(left, right, got):
        half = left.shape[1] // 2
        left, got = order.hold(left, got)
        own = mm(lax.dynamic_slice_in_dim(left, parity * half, half, 1), right, 0, 0)
        own = (own + got.astype(F32)).astype(BF)
        order.mark(own)
        return own

    def enqueue(own, rows):
        rows = min(rows, own.shape[0])
        return [chain.feed(own[i : i + rows]) for i in range(0, own.shape[0], rows)]

    def collect(numbers, axis=0):
        own = jnp.concatenate([chain.done[n] for n in numbers], axis=axis)
        return own, swap(own, "replica", 1)

    def blocks_of(value):
        return [value[s * local_rows : (s + 1) * local_rows] for s in range(group_size)]

    down_got = other_half(hidden, grad_rows)
    gate_got = other_half(grad_gate, mlp_rows)
    down_numbers = enqueue(own_half(hidden, grad_rows, down_got), CHUNK)

    chain.start(order)
    grad_gate_up = jnp.stack(order.hold(grad_gate, grad_up), axis=1)
    back_term = jnp.einsum("tkn,nkd->td", grad_gate_up, w_in, preferred_element_type=F32)
    order.mark(back_term)
    grad_scatter = Scatter(blocks_of(back_term), "group")
    grad_scatter.send()
    chain.fold(order)

    chain.start(order)
    gate_numbers = enqueue(own_half(grad_gate, mlp_rows, gate_got), CHUNK)
    grad_scatter.relay(order.hold)
    order.mark(*grad_scatter.total[1:])
    up_got = other_half(grad_up, mlp_rows)
    chain.fold(order)

    chain.start(order)
    up_numbers = enqueue(own_half(grad_up, mlp_rows, up_got), CHUNK)
    attended_cols = exchange_columns(order.hold(attended), "group", group_index)
    feed_term = mm(order.hold(hidden), w_down, 1, 0)
    order.mark(feed_term)
    chain.fold(order)

    chain.start(order)
    grad_normed = grad_scatter.receive(order.hold)
    grad_mid_norm, gain_mid_term = norm_backward(grad_normed, unit_mid, scale_mid, gain_mid_float)
    grad_middle = grad_out.astype(F32) + grad_mid_norm
    grad_branch = grad_middle.astype(BF)
    grad_attended = mm(grad_branch, out_full, 1, 1).astype(BF)
    order.mark(grad_attended)
    branch_gather = Gather(grad_branch, "group")
    chain.fold(order)

    pairs = kv_width // 128
    parts = 2 if pairs % 2 == 0 else 1
    grads = []
    for i in range(parts):
        chain.start(order)
        grads.append(
            attention_backward(
                bounds,
                queries,
                attended,
                order.hold(grad_attended),
                kv_all,
                logs,
                starts,
                i * (pairs // parts),
                pairs // parts,
            )
        )
        order.mark(grads[-1][0])
        if i == parts - 1:
            branch_blocks = branch_gather.relay(order.hold)
            kv_parts = [g[1] for g in grads] + [g[2] for g in grads]
            kv_terms = [
                jnp.concatenate(
                    [
                        lax.dynamic_slice_in_dim(part, (group_index ^ s) * local_rows, local_rows, 0)
                        for part in kv_parts
                    ],
                    axis=1,
                ).astype(BF if s else F32)
                for s in range(group_size)
            ]
            kv_scatter = Scatter(kv_terms, "group")
            kv_scatter.send()
            order.mark(*kv_terms)
        chain.fold(order)
    grad_query = jnp.concatenate([g[0] for g in grads], axis=1)

    chain.start(order)
    kv_scatter.relay(order.hold)
    order.mark(*kv_scatter.total[1:])
    attended_rows = jnp.concatenate(attended_cols, axis=0)
    branch_rows = jnp.concatenate(branch_blocks, axis=0)
    out_got = other_half(attended_rows, branch_rows)
    out_own = own_half(attended_rows, branch_rows, out_got)
    out_numbers = enqueue(out_own, CHUNK)
    kv_grad = kv_scatter.receive(order.hold)
    grad_projected = pl.pallas_call(
        functools.partial(rope_backward_body, width, kv_width),
        in_specs=whole(grad_query, kv_grad, cosine, sine),
        out_specs=whole(projected)[0],
        out_shape=jax.ShapeDtypeStruct((local_rows, qkv_cols), BF),
        name="rope_backward",
    )(grad_query, kv_grad, cosine, sine)
    order.mark(grad_projected)
    proj_gather = Gather(grad_projected, "group")
    chain.fold(order)

    down_own, down_other = collect(down_numbers)
    chain.start(order)
    down_own, down_other = order.hold(down_own, down_other)
    down_sum = place_halves(parity, down_own, down_other)
    order.mark(down_sum)
    chain.fold(order)

    chain.start(order)
    proj_blocks = proj_gather.relay(order.hold)
    grad_normed_in = mm(order.hold(grad_projected), qkv_full, 1, 1)
    grad_in_norm, gain_in_term = norm_backward(grad_normed_in, unit_in, scale_in, gain_in_float)
    grad_input = (grad_middle + grad_in_norm).astype(BF)
    order.mark(grad_input)
    gain_terms = jnp.stack([gain_in_term, gain_mid_term])
    parts = exchange_columns(gain_terms, "group", group_index)
    gain_rounds = [1 << bit for bit in range((lax.axis_size("replica") - 1).bit_length())]
    gain_got = parts[1:]
    gain_sum = parts[0]
    chain.fold(order)

    chain.start(order)
    proj_rows = jnp.concatenate(proj_blocks, axis=0)
    normed_rows = jnp.concatenate(normed_cols, axis=0)
    proj_rows, normed_rows = order.hold(proj_rows, normed_rows)
    qkv_got = other_half(normed_rows, proj_rows)
    qkv_own = own_half(normed_rows, proj_rows, qkv_got)
    qkv_numbers = [chain.feed(qkv_own[:, :width]), chain.feed(qkv_own[:, width:])]
    feed_scatter = Scatter(blocks_of(after(feed_term, qkv_own)), "group")
    feed_scatter.send()
    chain.fold(order)

    chain.start(order)
    gain_sum = sum(as_list(order.hold(*gain_got)), gain_sum)
    order.mark(gain_sum)
    if gain_rounds:
        gain_got = [swap(gain_sum, "replica", gain_rounds.pop(0))]
    feed_scatter.relay(order.hold)
    order.mark(*feed_scatter.total[1:])
    chain.fold(order)

    chain.start(order)
    gain_sum = sum(as_list(order.hold(*gain_got)), gain_sum)
    order.mark(gain_sum)
    if gain_rounds:
        gain_got = [swap(gain_sum, "replica", gain_rounds.pop(0))]
    output = (middle + feed_scatter.receive(order.hold)).astype(BF)
    order.mark(output)
    chain.fold(order)

    while chain.length == 4 and len(chain.done) < max(up_numbers) + 1:
        chain.start(order)
        if gain_rounds:
            gain_sum = sum(as_list(order.hold(*gain_got)), gain_sum)
            order.mark(gain_sum)
            gain_got = [swap(gain_sum, "replica", gain_rounds.pop(0))]
        chain.fold(order)
    gate_own, gate_other = collect(gate_numbers)
    up_own, up_other = collect(up_numbers)
    chain.start(order)
    gate_own, gate_other, up_own, up_other = order.hold(gate_own, gate_other, up_own, up_other)
    in_sum = place_halves(parity, gate_own, gate_other, up_own, up_other)
    order.mark(in_sum)
    chain.fold(order)
    out_sum = None
    while chain.length == 4 and len(chain.done) < len(chain.queue):
        ready = out_sum is None and all(n in chain.done for n in out_numbers)
        if ready:
            out_own, out_other = collect(out_numbers)
        chain.start(order)
        if ready:
            out_own, out_other = order.hold(out_own, out_other)
            out_sum = place_halves(parity, out_own, out_other)
            order.mark(out_sum)
        chain.fold(order)
    if out_sum is None:
        out_sum = place_halves(parity, *collect(out_numbers))
    while gain_rounds:
        gain_sum = sum(gain_got, gain_sum)
        gain_got = [swap(gain_sum, "replica", gain_rounds.pop(0))]
    gain_sum = sum(gain_got, gain_sum)
    qkv_sum = place_halves(parity, *collect(qkv_numbers, 1))

    return (
        output[None],
        grad_input[None],
        gain_sum[0],
        qkv_sum,
        out_sum,
        gain_sum[1],
        in_sum,
        down_sum,
    )


def solution(mesh):
    return jax.shard_map(
        shards,
        mesh=mesh,
        in_specs=(
            P("replica", "group", None),
            P("replica", None),
            P("replica", "group"),
            P("group"),
            P("group", None),
            P("group", None),
            P("group"),
            P("group", None, None),
            P("group", None),
            P("replica", "group", None),
        ),
        out_specs=(
            P("replica", "group", None),
            P("replica", "group", None),
            P("group"),
            P("group", None),
            P("group", None),
            P("group"),
            P("group", None, None),
            P("group", None),
        ),
        check_vma=False,
    )
```

```python
import functools
import math

import jax
import jax.numpy as jnp
from jax import lax
from jax.experimental import pallas as pl
from jax.experimental.pallas import tpu as pltpu
from jax.sharding import PartitionSpec as P

HEAD = 64
EPS = 1e-05
ROPE_BASE = 500000.0
ROPE_FACTOR = 32.0
LOW_FACTOR = 1.0
HIGH_FACTOR = 4.0
OLD_CONTEXT = 8192.0
BF = jnp.bfloat16
F32 = jnp.float32
NEG = -1e30

CHUNK = 256


def rope_frequency(head_size):
    half = head_size // 2
    exponent = jnp.arange(half).astype(jnp.float32) * (2.0 / head_size)
    frequency = jnp.power(jnp.float32(ROPE_BASE), -exponent)
    wavelength = 2.0 * math.pi / frequency
    smooth = (OLD_CONTEXT / wavelength - LOW_FACTOR) / (HIGH_FACTOR - LOW_FACTOR)
    blended = (1.0 - smooth) * frequency / ROPE_FACTOR + smooth * frequency
    slow = jnp.where(wavelength > OLD_CONTEXT / LOW_FACTOR, frequency / ROPE_FACTOR, blended)
    return jnp.where(wavelength < OLD_CONTEXT / HIGH_FACTOR, frequency, slow)


def rope_tables(position, head_size):
    frequency = rope_frequency(head_size)
    angle = position.astype(jnp.float32)[:, None] * frequency[None, :]
    return (jnp.cos(angle), jnp.sin(angle))


def rms_scale(values):
    return lax.rsqrt(jnp.mean(values * values, axis=-1, keepdims=True) + EPS)


def norm_backward(grad_normed, unit, scale, gain):
    grad_unit = grad_normed * gain
    grad_input = scale * (grad_unit - unit * jnp.mean(grad_unit * unit, axis=-1, keepdims=True))
    return (grad_input, jnp.sum(grad_normed * unit, axis=0))


def mm(a, b, ca, cb):
    return lax.dot_general(a, b, (((ca,), (cb,)), ((), ())), preferred_element_type=F32)


def swap(value, axis, mask):
    return lax.ppermute(value, axis, [(i, i ^ mask) for i in range(lax.axis_size(axis))])


def bit_list(number):
    return [1 << b for b in range(number.bit_length()) if number >> b & 1]


def pieces_of(rows, number):
    bits = bit_list(number)
    while rows % (16 * len(bits)):
        bits = bits[:-1]
    step = rows // len(bits)
    return [(bit, i * step, step) for i, bit in enumerate(bits)]


def as_list(values):
    return list(values) if isinstance(values, (tuple, list)) else [values]


class Order:
    def __init__(self):
        self.marked = ()

    def hold(self, *values):
        held = lax.optimization_barrier((*values, *self.marked))[: len(values)] if self.marked else values
        return held[0] if len(held) == 1 else held

    def mark(self, *values):
        self.marked = values


class Gather:
    def __init__(self, own, axis):
        self.axis, self.size = axis, lax.axis_size(axis)
        self.rows = own.shape[0]
        self.blocks = {0: own}
        for s in range(1, self.size):
            if len(bit_list(s)) == 1:
                self.blocks[s] = swap(own, axis, s)

    def relay(self, hold=lambda *v: v):
        numbers = sorted(self.blocks)[1:]
        held = hold(*[self.blocks[s] for s in numbers]) if numbers else ()
        if len(numbers) == 1:
            held = (held[0] if isinstance(held, tuple) else held,)
        self.blocks.update(zip(numbers, held))
        for s in range(1, self.size):
            if s not in self.blocks:
                parts = [
                    swap(self.blocks[s ^ bit][start : start + size], self.axis, bit)
                    for bit, start, size in pieces_of(self.rows, s)
                ]
                self.blocks[s] = parts[0] if len(parts) == 1 else jnp.concatenate(parts, axis=0)
        return [self.blocks[s] for s in range(self.size)]


def gather_blocks(own, axis):
    return Gather(own, axis).relay()


class Scatter:
    def __init__(self, terms, axis):
        self.total, self.axis = list(terms), axis
        self.level = max(len(bit_list(s)) for s in range(len(terms)))

    def send(self):
        self.flying = []
        for s in range(1, len(self.total)):
            if len(bit_list(s)) == self.level:
                sent = self.total[s].astype(BF)
                for bit, start, size in pieces_of(sent.shape[0], s):
                    self.flying.append((s ^ bit, start, size, swap(sent[start : start + size], self.axis, bit)))
        self.level -= 1

    def receive(self, hold=lambda *v: v):
        got = hold(*[f[3] for f in self.flying])
        got = got if isinstance(got, (tuple, list)) else (got,)
        for (s, start, size, _), value in zip(self.flying, got):
            into, value = self.total[s], value.astype(F32)
            if size == into.shape[0]:
                self.total[s] = into + value
            else:
                rows = [into[:start], into[start : start + size] + value, into[start + size :]]
                self.total[s] = jnp.concatenate([r for r in rows if r.shape[0]], axis=0)
        return self.total[0]

    def relay(self, hold=lambda *v: v):
        while self.level:
            self.receive(hold)
            self.send()


def exchange_columns(value, axis, index):
    size = lax.axis_size(axis)
    width = value.shape[1] // size
    out = [lax.dynamic_slice_in_dim(value, index * width, width, 1)]
    for s in range(1, size):
        part = lax.dynamic_slice_in_dim(value, (index ^ s) * width, width, 1)
        out.append(swap(part, axis, s))
    return out


def chain_sum(value, axis, position, length):
    half = length // 2

    def hop(value, moves):
        return lax.ppermute(value, axis, [(2 * a + c, 2 * b + c) for a, b in moves for c in (0, 1)])

    def add(a, b):
        return (a.astype(F32) + b.astype(F32)).astype(BF)

    total = value
    last = length - 1
    for step in range(half - 1):
        total = add(total, hop(total, [(step, step + 1), (last - step, last - step - 1)]))
    total = add(total, hop(total, [(half - 1, half), (half, half - 1)]))
    for step in reversed(range(half - 1)):
        got = hop(total, [(step + 1, step), (last - step - 1, last - step)])
        total = jnp.where((position == step) | (position == last - step), got, total)
    return total


def half_lanes(shape):
    return lax.broadcasted_iota(jnp.int32, shape, 1) % 128 < HEAD


def place(value, source, target):
    if source != target:
        value = pltpu.roll(value, HEAD, 1)
    low = half_lanes(value.shape)
    return jnp.where(low if target == 0 else ~low, value, 0.0)


def turn(value, cosine, sine):
    lane = lax.broadcasted_iota(jnp.int32, value.shape, 1) % HEAD
    partner = jnp.where(lane < HEAD // 2, pltpu.roll(value, 128 - HEAD // 2, 1), pltpu.roll(value, HEAD // 2, 1))
    return value * cosine + partner * sine


def rope_forward_body(width, kv_width, proj_ref, cos_ref, sin_ref, q_ref, kv_ref):
    cosine, sine = cos_ref[...], sin_ref[...]
    for at in range(0, width, 128):
        q_ref[:, at : at + 128] = (turn(proj_ref[:, at : at + 128], cosine, sine) * HEAD**-0.5).astype(BF)
    for at in range(0, kv_width, 128):
        kv_ref[:, at : at + 128] = turn(proj_ref[:, width + at : width + at + 128], cosine, sine).astype(BF)
    kv_ref[:, kv_width:] = proj_ref[:, width + kv_width :].astype(BF)


def rope_backward_body(width, kv_width, gq_ref, gkv_ref, cos_ref, sin_ref, out_ref):
    cosine, sine = cos_ref[...], -sin_ref[...]
    for at in range(0, width, 128):
        out_ref[:, at : at + 128] = turn(gq_ref[:, at : at + 128], cosine, sine).astype(BF)
    for at in range(0, kv_width, 128):
        out_ref[:, width + at : width + at + 128] = turn(gkv_ref[:, at : at + 128], cosine, sine).astype(BF)
    out_ref[:, width + kv_width :] = gkv_ref[:, kv_width:].astype(BF)


def whole(*arrays):
    return [pl.BlockSpec(a.shape, lambda *_: (0,) * a.ndim) for a in arrays]


def attention_forward_body(rows, per_kv, bounds_ref, q_ref, k_ref, v_ref, start_ref, out_ref, lse_ref):
    first, low_block, last_block = bounds_ref[0], bounds_ref[1], bounds_ref[2]
    row = first + lax.broadcasted_iota(jnp.int32, (rows, rows), 1)
    key_in_block = lax.broadcasted_iota(jnp.int32, (rows, rows), 0)
    start = start_ref[...]
    groups = [[(c, j, e) for c in range(2) for j in range(per_kv // 2) for e in range(2)]]
    for these in groups:
            heads = []
            for c, j, e in these:
                at = (c * (per_kv // 2) + j) * 128
                heads.append(place(q_ref[:, at : at + 128].astype(F32), e, c).astype(BF))

            def block(i, carry):
                kb = last_block - i
                rows_of = pl.ds(pl.multiple_of(kb * rows, rows), rows)
                k_block = k_ref[rows_of, :]
                v_block = v_ref[rows_of, :]
                key = key_in_block + kb * rows
                mask = (key <= row) & (key >= start)
                new = []
                scores = [jnp.where(mask, mm(k_block, h, 1, 1), NEG) for h in heads]
                for e, s in enumerate(scores):
                    top, total, mixed = carry[3 * e : 3 * e + 3]
                    raised = jnp.maximum(top, jnp.max(s, axis=0, keepdims=True))
                    fade = jnp.exp(top - raised)
                    p = jnp.exp(s - raised)
                    total = total * fade + jnp.sum(p, axis=0, keepdims=True)
                    new += [raised, total, mixed * fade + mm(v_block, p.astype(BF), 0, 0)]
                return tuple(new)

            begin = (jnp.full((1, rows), NEG, F32), jnp.zeros((1, rows), F32), jnp.zeros((128, rows), F32))
            carry = lax.fori_loop(0, last_block + 1 - low_block, block, begin * len(these))
            parts = {}
            for i, (c, j, e) in enumerate(these):
                index = c * per_kv + 2 * j + e
                top, total, mixed = carry[3 * i : 3 * i + 3]
                lse_ref[index : index + 1, :] = top + jnp.log(total)
                parts[c, j, e] = mixed[c * HEAD : (c + 1) * HEAD] / total
            for c, j, e in these:
                if e == 0:
                    at = (c * (per_kv // 2) + j) * 128
                    both = jnp.concatenate([parts[c, j, 0], parts[c, j, 1]], axis=0)
                    out_ref[:, at : at + 128] = jnp.transpose(both).astype(BF)


def attention_backward_body(
    rows, per_kv, bounds_ref, q_ref, o_ref, g_ref, k_ref, v_ref, lse_ref, start_ref, gq_ref, gk_ref, gv_ref
):
    first, low_block, last_block = bounds_ref[0], bounds_ref[1], bounds_ref[2]
    row = first + lax.broadcasted_iota(jnp.int32, (rows, rows), 1)
    key_in_block = lax.broadcasted_iota(jnp.int32, (rows, rows), 0)
    start = start_ref[...]
    gk_ref[...] = jnp.zeros(gk_ref.shape, F32)
    gv_ref[...] = jnp.zeros(gv_ref.shape, F32)
    groups = [[(c, j) for c in range(2) for j in range(per_kv // 2)]]
    for these in groups:
        info = []
        for c, j in these:
            at = (c * (per_kv // 2) + j) * 128
            q_pair = q_ref[:, at : at + 128].astype(F32)
            g_pair = g_ref[:, at : at + 128].astype(F32)
            product = jnp.transpose(g_pair * o_ref[:, at : at + 128].astype(F32))
            for e in range(2):
                index = c * per_kv + 2 * j + e
                info.append(
                    (
                        place(q_pair, e, c).astype(BF),
                        place(g_pair, e, c).astype(BF),
                        jnp.sum(product[e * HEAD : (e + 1) * HEAD], axis=0, keepdims=True),
                        lse_ref[index : index + 1, :],
                    )
                )

        def block(kb, carry):
            rows_of = pl.ds(pl.multiple_of(kb * rows, rows), rows)
            k_block = k_ref[rows_of, :]
            v_block = v_ref[rows_of, :]
            key = key_in_block + kb * rows
            mask = (key <= row) & (key >= start)
            new = []
            grad_k = gk_ref[rows_of, :]
            grad_v = gv_ref[rows_of, :]
            for (q_head, g_head, inner, logs), grad_q in zip(info, carry):
                s = jnp.where(mask, mm(k_block, q_head, 1, 1), NEG)
                p = jnp.exp(s - logs)
                grad_p = mm(v_block, g_head, 1, 1)
                grad_s = (p * (grad_p - inner)).astype(BF)
                grad_v = grad_v + mm(p.astype(BF), g_head, 1, 0)
                grad_k = grad_k + mm(grad_s, q_head, 1, 0)
                new.append(grad_q + mm(grad_s, k_block, 0, 0))
            gk_ref[rows_of, :] = grad_k
            gv_ref[rows_of, :] = grad_v
            return tuple(new)

        zero = jnp.zeros((rows, 128), F32)
        grads = lax.fori_loop(low_block, last_block + 1, block, (zero,) * len(info))
        for i, (c, j) in enumerate(these):
            at = (c * (per_kv // 2) + j) * 128
            total = place(grads[2 * i], c, 0) + place(grads[2 * i + 1], c, 1)
            gq_ref[:, at : at + 128] = total * HEAD**-0.5


def attention_forward(bounds, queries, keys_values, start):
    rows, width = queries.shape
    length, kv2 = keys_values.shape
    pairs = kv2 // 2 // 128
    wide = width // pairs
    per_kv = wide // (2 * HEAD)
    spec = pltpu.PrefetchScalarGridSpec(
        num_scalar_prefetch=1,
        grid=(pairs,),
        in_specs=[
            pl.BlockSpec((rows, wide), lambda i, b: (0, i)),
            pl.BlockSpec((length, 128), lambda i, b: (0, i)),
            pl.BlockSpec((length, 128), lambda i, b: (0, i + pairs)),
            pl.BlockSpec((1, rows), lambda i, b: (0, 0)),
        ],
        out_specs=[
            pl.BlockSpec((rows, wide), lambda i, b: (0, i)),
            pl.BlockSpec((2 * per_kv, rows), lambda i, b: (i, 0)),
        ],
    )
    return pl.pallas_call(
        functools.partial(attention_forward_body, rows, per_kv),
        grid_spec=spec,
        out_shape=[
            jax.ShapeDtypeStruct((rows, width), BF),
            jax.ShapeDtypeStruct((2 * per_kv * pairs, rows), F32),
        ],
        cost_estimate=pl.CostEstimate(
            flops=8 * rows * length * width, transcendentals=rows * length * width // HEAD, bytes_accessed=8 * rows * width
        ),
        name="attention_forward",
    )(bounds, queries, keys_values, keys_values, start[None])


def attention_backward(bounds, queries, attended, grad, keys_values, logs, start, base, count):
    rows, width = queries.shape
    length, kv2 = keys_values.shape
    pairs = kv2 // 2 // 128
    wide = width // pairs
    per_kv = wide // (2 * HEAD)
    row_block = pl.BlockSpec((rows, wide), lambda i, b: (0, i + base))
    spec = pltpu.PrefetchScalarGridSpec(
        num_scalar_prefetch=1,
        grid=(count,),
        in_specs=[
            row_block,
            row_block,
            row_block,
            pl.BlockSpec((length, 128), lambda i, b: (0, i + base)),
            pl.BlockSpec((length, 128), lambda i, b: (0, i + base + pairs)),
            pl.BlockSpec((2 * per_kv, rows), lambda i, b: (i + base, 0)),
            pl.BlockSpec((1, rows), lambda i, b: (0, 0)),
        ],
        out_specs=[
            pl.BlockSpec((rows, wide), lambda i, b: (0, i)),
            pl.BlockSpec((length, 128), lambda i, b: (0, i)),
            pl.BlockSpec((length, 128), lambda i, b: (0, i)),
        ],
    )
    return pl.pallas_call(
        functools.partial(attention_backward_body, rows, per_kv),
        grid_spec=spec,
        out_shape=[
            jax.ShapeDtypeStruct((rows, wide * count), F32),
            jax.ShapeDtypeStruct((length, 128 * count), F32),
            jax.ShapeDtypeStruct((length, 128 * count), F32),
        ],
        cost_estimate=pl.CostEstimate(
            flops=20 * rows * length * wide * count,
            transcendentals=rows * length * wide * count // HEAD,
            bytes_accessed=8 * rows * width,
        ),
        name="attention_backward",
    )(bounds, queries, attended, grad, keys_values, keys_values, logs, start[None])
class Chain:
    def __init__(self, axis, position, length):
        self.axis, self.position, self.length = axis, position, length
        self.queue, self.sums, self.done = [], {}, {}
        self.tick = 0
        self.flying = None

    def feed(self, chunk):
        if self.length != 4:
            self.done[len(self.queue)] = chain_sum(chunk, self.axis, self.position, self.length)
        self.queue.append(chunk)
        return len(self.queue) - 1

    def hop(self, value, moves, idle=()):
        pairs = [(2 * a + c, 2 * b + c) for a, b in moves for c in (0, 1)]
        return lax.ppermute(value, self.axis, pairs + [(2 * a + c, 2 * a + 1 - c) for a in idle for c in (0, 1)])

    def start(self, order):
        t = self.tick
        outer = (self.position == 0) | (self.position == 3)
        fresh = self.queue[t] if t < len(self.queue) else None
        across = self.sums.get(t - 1)
        final = self.sums.get((t - 2, 1))
        self.flying = None
        if self.length != 4 or (fresh is None and across is None and final is None):
            return
        if fresh is None:
            outgoing = final
        elif final is None:
            outgoing = fresh
        else:
            shape = tuple(map(max, zip(fresh.shape, final.shape)))
            outgoing = jnp.where(outer, widen(fresh, shape), widen(final, shape))
        sent = [v for v in (outgoing, across) if v is not None]
        held = order.hold(*sent)
        held = list(held) if len(sent) > 1 else [held]
        got = []
        if outgoing is not None:
            got.append(self.hop(held.pop(0), [(0, 1), (1, 0), (2, 3), (3, 2)]))
        if across is not None:
            got.append(self.hop(held.pop(0), [(1, 2), (2, 1)], (0, 3)))
        self.flying = (outer, fresh, across, final, got)

    def fold(self, order):
        t = self.tick
        self.tick += 1
        if self.flying is None:
            return
        outer, fresh, across, final, got = self.flying
        held = order.hold(*got)
        held = list(held) if len(got) > 1 else [held]
        marks = []
        if fresh is not None or final is not None:
            value = held.pop(0)
            if fresh is not None:
                self.sums[t] = rounded_sum(fresh, cut(value, fresh.shape))
                marks.append(self.sums[t])
            if final is not None:
                self.done[t - 2] = jnp.where(outer, cut(value, final.shape), final)
        if across is not None:
            self.sums[t - 1, 1] = rounded_sum(across, held.pop(0))
            marks.append(self.sums[t - 1, 1])
        order.mark(*(marks or held or got))


def widen(value, shape):
    pads = [(0, want - have) for want, have in zip(shape, value.shape)]
    return jnp.pad(value, pads) if any(p[1] for p in pads) else value


def cut(value, shape):
    return value[: shape[0], : shape[1]]


def after(value, *others):
    return lax.optimization_barrier((value, *others))[0]


def rounded_sum(a, b):
    return (a.astype(F32) + b.astype(F32)).astype(BF)


def place_rows_body(parity_ref, own_ref, other_ref, out_ref):
    own = pl.program_id(0) < pl.num_programs(0) // 2

    @pl.when(own)
    def _():
        out_ref[...] = own_ref[...].astype(F32)

    @pl.when(~own)
    def _():
        out_ref[...] = other_ref[...].astype(F32)


def place_pairs_body(parity_ref, own_a_ref, other_a_ref, own_b_ref, other_b_ref, out_ref):
    own = pl.program_id(0) < pl.num_programs(0) // 2

    @pl.when(own)
    def _():
        out_ref[:, 0, :] = own_a_ref[...].astype(F32)
        out_ref[:, 1, :] = own_b_ref[...].astype(F32)

    @pl.when(~own)
    def _():
        out_ref[:, 0, :] = other_a_ref[...].astype(F32)
        out_ref[:, 1, :] = other_b_ref[...].astype(F32)


def place_halves(parity, *halves):
    rows, width = halves[0].shape
    size = 128 if rows % 128 == 0 else rows
    count = rows // size
    own = pl.BlockSpec((size, width), lambda i, p: (jnp.minimum(i, count - 1), 0))
    other = pl.BlockSpec((size, width), lambda i, p: (jnp.maximum(i - count, 0), 0))

    def spot(i, p):
        return jnp.where(i < count, p[0] * count + i, (1 - p[0]) * count + i - count)

    if len(halves) == 2:
        body, shape = place_rows_body, (2 * rows, width)
        out = pl.BlockSpec((size, width), lambda i, p: (spot(i, p), 0))
    else:
        body, shape = place_pairs_body, (2 * rows, 2, width)
        out = pl.BlockSpec((size, 2, width), lambda i, p: (spot(i, p), 0, 0))
    spec = pltpu.PrefetchScalarGridSpec(
        num_scalar_prefetch=1, grid=(2 * count,), in_specs=[own, other] * (len(halves) // 2), out_specs=out
    )
    return pl.pallas_call(
        body,
        grid_spec=spec,
        out_shape=jax.ShapeDtypeStruct(shape, F32),
        cost_estimate=pl.CostEstimate(
            flops=rows * width * 2, transcendentals=0, bytes_accessed=6 * rows * width * len(halves)
        ),
        name="place_halves",
    )(parity[None], *halves)


def shards(tokens, segments, positions, norm_in, w_qkv, w_out, norm_mid, w_in, w_down, cotangent):
    inputs = tokens[0]
    local_rows, width = inputs.shape
    qkv_cols = w_qkv.shape[1]
    kv_width = (qkv_cols - width) // 2
    group_size = lax.axis_size("group")
    group_index = lax.axis_index("group")
    replica_index = lax.axis_index("replica")
    parity = replica_index % 2
    position = replica_index // 2
    length = lax.axis_size("replica") // 2
    first_row = group_index * local_rows
    seq_ids = segments[0]
    seq_len = seq_ids.shape[0]

    def gather_weight(weight, *others):
        rows = weight.shape[0]
        half = rows // 2
        mine = lax.dynamic_slice_in_dim(weight, parity * half, half, 0)
        if others:
            mine = after(mine, *others)
        full = jnp.zeros((rows * group_size, weight.shape[1]), weight.dtype)
        blocks = gather_blocks(mine, "group")
        for s, block in enumerate(blocks):
            base = (group_index ^ s) * rows
            if s == 0:
                full = lax.dynamic_update_slice_in_dim(full, weight, base, 0)
                continue
            full = lax.dynamic_update_slice_in_dim(full, block, base + parity * half, 0)
            other = swap(block, "replica", 1)
            full = lax.dynamic_update_slice_in_dim(full, other, base + (1 - parity) * half, 0)
        return full, blocks[-1]

    def gather_rows(own):
        rows = own.shape[0]
        full = jnp.zeros((rows * group_size, own.shape[1]), own.dtype)
        for s, block in enumerate(gather_blocks(own, "group")):
            full = lax.dynamic_update_slice_in_dim(full, block, (group_index ^ s) * rows, 0)
        return full

    qkv_full, qkv_mark = gather_weight(w_qkv)
    gains = jnp.stack([norm_in, norm_mid])
    gain_full = jnp.zeros((2, width), BF)
    gain_full = lax.dynamic_update_slice_in_dim(gain_full, gains, group_index * norm_in.shape[0], 1)
    for s in range(1, group_size):
        gain_full = lax.dynamic_update_slice_in_dim(
            gain_full, swap(gains, "group", s), (group_index ^ s) * norm_in.shape[0], 1
        )
    gain_in_float = gain_full[0].astype(F32)
    gain_mid_float = gain_full[1].astype(F32)

    own_ids = lax.dynamic_slice_in_dim(seq_ids, first_row, local_rows)
    starts = jnp.sum((seq_ids[None, :] < own_ids[:, None]).astype(jnp.int32), axis=1)
    bounds = jnp.stack([first_row, starts[0] // local_rows, group_index]).astype(jnp.int32)
    cosine, sine = rope_tables(positions[0], HEAD)
    cosine = jnp.concatenate([cosine] * 4, axis=1)
    sine = jnp.concatenate([-sine, sine] * 2, axis=1)
    input_float = inputs.astype(F32)
    scale_in = rms_scale(input_float)
    unit_in = input_float * scale_in
    normed_in = (unit_in * gain_in_float).astype(BF)
    projected = mm(normed_in, qkv_full, 1, 0)
    queries, kv_own = pl.pallas_call(
        functools.partial(rope_forward_body, width, kv_width),
        in_specs=whole(projected, cosine, sine),
        out_specs=whole(inputs, inputs[:, : 2 * kv_width]),
        out_shape=[
            jax.ShapeDtypeStruct((local_rows, width), BF),
            jax.ShapeDtypeStruct((local_rows, 2 * kv_width), BF),
        ],
        name="rope_forward",
    )(projected, cosine, sine)
    kv_all = gather_rows(kv_own)
    out_full, _ = gather_weight(w_out, qkv_mark)
    grad_out = cotangent[0]
    grad_blocks = gather_blocks(after(grad_out, kv_all), "group")

    attended, logs = attention_forward(bounds, queries, kv_all, starts)
    middle = input_float + mm(attended, out_full, 1, 0)
    scale_mid = rms_scale(middle)
    unit_mid = middle * scale_mid
    normed_mid = (unit_mid * gain_mid_float).astype(BF)

    mlp_rows = jnp.concatenate(gather_blocks(normed_mid, "group"), axis=0)
    grad_rows = jnp.concatenate(grad_blocks, axis=0)
    grad_hidden = lax.optimization_barrier(mm(grad_rows, w_down, 1, 1))
    gate_up = jnp.einsum("td,nkd->tkn", mlp_rows, w_in, preferred_element_type=F32)
    normed_cols = exchange_columns(after(normed_in, mlp_rows), "group", group_index)
    gate, up = gate_up[:, 0], gate_up[:, 1]
    sigma = jax.nn.sigmoid(gate)
    hidden = (gate * sigma * up).astype(BF)
    grad_gate = (grad_hidden * up * (sigma * (1.0 + gate * (1.0 - sigma)))).astype(BF)
    grad_up = (grad_hidden * gate * sigma).astype(BF)

    order = Order()
    chain = Chain("replica", position, length)

    def other_half(left, right):
        half = left.shape[1] // 2
        left = order.hold(left)
        term = mm(lax.dynamic_slice_in_dim(left, (1 - parity) * half, half, 1), right, 0, 0).astype(BF)
        order.mark(term)
        return swap(term, "replica", 1)

    def own_half(left, right, got):
        half = left.shape[1] // 2
        left, got = order.hold(left, got)
        own = mm(lax.dynamic_slice_in_dim(left, parity * half, half, 1), right, 0, 0)
        own = (own + got.astype(F32)).astype(BF)
        order.mark(own)
        return own

    def enqueue(own, rows):
        rows = min(rows, own.shape[0])
        return [chain.feed(own[i : i + rows]) for i in range(0, own.shape[0], rows)]

    def collect(numbers, axis=0):
        own = jnp.concatenate([chain.done[n] for n in numbers], axis=axis)
        return own, swap(own, "replica", 1)

    def blocks_of(value):
        return [value[s * local_rows : (s + 1) * local_rows] for s in range(group_size)]

    down_got = other_half(hidden, grad_rows)
    gate_got = other_half(grad_gate, mlp_rows)
    down_numbers = enqueue(own_half(hidden, grad_rows, down_got), CHUNK)

    chain.start(order)
    grad_gate_up = jnp.stack(order.hold(grad_gate, grad_up), axis=1)
    back_term = jnp.einsum("tkn,nkd->td", grad_gate_up, w_in, preferred_element_type=F32)
    order.mark(back_term)
    grad_scatter = Scatter(blocks_of(back_term), "group")
    grad_scatter.send()
    chain.fold(order)

    chain.start(order)
    gate_numbers = enqueue(own_half(grad_gate, mlp_rows, gate_got), CHUNK)
    grad_scatter.relay(order.hold)
    order.mark(*grad_scatter.total[1:])
    up_got = other_half(grad_up, mlp_rows)
    chain.fold(order)

    chain.start(order)
    up_numbers = enqueue(own_half(grad_up, mlp_rows, up_got), CHUNK)
    attended_cols = exchange_columns(order.hold(attended), "group", group_index)
    feed_term = mm(order.hold(hidden), w_down, 1, 0)
    order.mark(feed_term)
    chain.fold(order)

    chain.start(order)
    grad_normed = grad_scatter.receive(order.hold)
    grad_mid_norm, gain_mid_term = norm_backward(grad_normed, unit_mid, scale_mid, gain_mid_float)
    grad_middle = grad_out.astype(F32) + grad_mid_norm
    grad_branch = grad_middle.astype(BF)
    grad_attended = mm(grad_branch, out_full, 1, 1).astype(BF)
    order.mark(grad_attended)
    branch_gather = Gather(grad_branch, "group")
    chain.fold(order)

    pairs = kv_width // 128
    parts = 2 if pairs % 2 == 0 else 1
    grads = []
    for i in range(parts):
        chain.start(order)
        grads.append(
            attention_backward(
                bounds,
                queries,
                attended,
                order.hold(grad_attended),
                kv_all,
                logs,
                starts,
                i * (pairs // parts),
                pairs // parts,
            )
        )
        order.mark(grads[-1][0])
        if i == parts - 1:
            branch_blocks = branch_gather.relay(order.hold)
            kv_parts = [g[1] for g in grads] + [g[2] for g in grads]
            kv_terms = [
                jnp.concatenate(
                    [
                        lax.dynamic_slice_in_dim(part, (group_index ^ s) * local_rows, local_rows, 0)
                        for part in kv_parts
                    ],
                    axis=1,
                ).astype(BF if s else F32)
                for s in range(group_size)
            ]
            kv_scatter = Scatter(kv_terms, "group")
            kv_scatter.send()
            order.mark(*kv_terms)
        chain.fold(order)
    grad_query = jnp.concatenate([g[0] for g in grads], axis=1)

    chain.start(order)
    kv_scatter.relay(order.hold)
    order.mark(*kv_scatter.total[1:])
    attended_rows = jnp.concatenate(attended_cols, axis=0)
    branch_rows = jnp.concatenate(branch_blocks, axis=0)
    out_got = other_half(attended_rows, branch_rows)
    out_own = own_half(attended_rows, branch_rows, out_got)
    out_numbers = enqueue(out_own, CHUNK)
    kv_grad = kv_scatter.receive(order.hold)
    grad_projected = pl.pallas_call(
        functools.partial(rope_backward_body, width, kv_width),
        in_specs=whole(grad_query, kv_grad, cosine, sine),
        out_specs=whole(projected)[0],
        out_shape=jax.ShapeDtypeStruct((local_rows, qkv_cols), BF),
        name="rope_backward",
    )(grad_query, kv_grad, cosine, sine)
    order.mark(grad_projected)
    proj_gather = Gather(grad_projected, "group")
    chain.fold(order)

    down_own, down_other = collect(down_numbers)
    chain.start(order)
    down_own, down_other = order.hold(down_own, down_other)
    down_sum = place_halves(parity, down_own, down_other)
    order.mark(down_sum)
    chain.fold(order)

    chain.start(order)
    proj_blocks = proj_gather.relay(order.hold)
    grad_normed_in = mm(order.hold(grad_projected), qkv_full, 1, 1)
    grad_in_norm, gain_in_term = norm_backward(grad_normed_in, unit_in, scale_in, gain_in_float)
    grad_input = (grad_middle + grad_in_norm).astype(BF)
    order.mark(grad_input)
    gain_terms = jnp.stack([gain_in_term, gain_mid_term])
    parts = exchange_columns(gain_terms, "group", group_index)
    gain_rounds = [1 << bit for bit in range((lax.axis_size("replica") - 1).bit_length())]
    gain_got = parts[1:]
    gain_sum = parts[0]
    chain.fold(order)

    chain.start(order)
    proj_rows = jnp.concatenate(proj_blocks, axis=0)
    normed_rows = jnp.concatenate(normed_cols, axis=0)
    proj_rows, normed_rows = order.hold(proj_rows, normed_rows)
    qkv_got = other_half(normed_rows, proj_rows)
    qkv_own = own_half(normed_rows, proj_rows, qkv_got)
    qkv_numbers = [chain.feed(qkv_own[:, :width]), chain.feed(qkv_own[:, width:])]
    feed_scatter = Scatter(blocks_of(after(feed_term, qkv_own)), "group")
    feed_scatter.send()
    chain.fold(order)

    chain.start(order)
    gain_sum = sum(as_list(order.hold(*gain_got)), gain_sum)
    order.mark(gain_sum)
    if gain_rounds:
        gain_got = [swap(gain_sum, "replica", gain_rounds.pop(0))]
    feed_scatter.relay(order.hold)
    order.mark(*feed_scatter.total[1:])
    chain.fold(order)

    chain.start(order)
    gain_sum = sum(as_list(order.hold(*gain_got)), gain_sum)
    order.mark(gain_sum)
    if gain_rounds:
        gain_got = [swap(gain_sum, "replica", gain_rounds.pop(0))]
    output = (middle + feed_scatter.receive(order.hold)).astype(BF)
    order.mark(output)
    chain.fold(order)

    while chain.length == 4 and len(chain.done) < max(up_numbers) + 1:
        chain.start(order)
        if gain_rounds:
            gain_sum = sum(as_list(order.hold(*gain_got)), gain_sum)
            order.mark(gain_sum)
            gain_got = [swap(gain_sum, "replica", gain_rounds.pop(0))]
        chain.fold(order)
    gate_own, gate_other = collect(gate_numbers)
    up_own, up_other = collect(up_numbers)
    chain.start(order)
    gate_own, gate_other, up_own, up_other = order.hold(gate_own, gate_other, up_own, up_other)
    in_sum = place_halves(parity, gate_own, gate_other, up_own, up_other)
    order.mark(in_sum)
    chain.fold(order)
    out_sum = None
    while chain.length == 4 and len(chain.done) < len(chain.queue):
        ready = out_sum is None and all(n in chain.done for n in out_numbers)
        if ready:
            out_own, out_other = collect(out_numbers)
        chain.start(order)
        if ready:
            out_own, out_other = order.hold(out_own, out_other)
            out_sum = place_halves(parity, out_own, out_other)
            order.mark(out_sum)
        chain.fold(order)
    if out_sum is None:
        out_sum = place_halves(parity, *collect(out_numbers))
    while gain_rounds:
        gain_sum = sum(gain_got, gain_sum)
        gain_got = [swap(gain_sum, "replica", gain_rounds.pop(0))]
    gain_sum = sum(gain_got, gain_sum)
    qkv_sum = place_halves(parity, *collect(qkv_numbers, 1))

    return (
        output[None],
        grad_input[None],
        gain_sum[0],
        qkv_sum,
        out_sum,
        gain_sum[1],
        in_sum,
        down_sum,
    )


def solution(mesh):
    return jax.shard_map(
        shards,
        mesh=mesh,
        in_specs=(
            P("replica", "group", None),
            P("replica", None),
            P("replica", "group"),
            P("group"),
            P("group", None),
            P("group", None),
            P("group"),
            P("group", None, None),
            P("group", None),
            P("replica", "group", None),
        ),
        out_specs=(
            P("replica", "group", None),
            P("replica", "group", None),
            P("group"),
            P("group", None),
            P("group", None),
            P("group"),
            P("group", None, None),
            P("group", None),
        ),
        check_vma=False,
    )
```
